16 devices in a mesh: col: 2 (over z), row: 8 (over y, x, core).
Axes of the slice: x: 2, y: 2, z: 2, core: 2. Of those that a mesh axis runs over, the one named last changes fastest.
Arguments:
- w_gate: float32 [4096, 10240], P('row', 'col')
- w_up: float32 [4096, 10240], P('row', 'col')
- w_down: float32 [10240, 4096], P('row', 'col')
- x_norm: bfloat16 [4096, 4096], P(None, 'row')
- x_act: bfloat16 [4096, 10240], P(None, 'row')
- dy_gate: bfloat16 [4096, 10240], P(None, 'col')
- dy_up: bfloat16 [4096, 10240], P(None, 'col')
- dy_down: bfloat16 [4096, 4096], P(None, 'col')
- r_gate: float32 [4096], P('row')
- c_gate: float32 [10240], P('col')
- r_up: float32 [4096], P('row')
- c_up: float32 [10240], P('col')
- r_down: float32 [10240], P('row')
- c_down: float32 [4096], P('col')
- hyper_params: float32 [3], replicated
Outputs:
- output 1: float32 [4096, 10240], P('row', 'col')
- output 2: float32 [4096, 10240], P('row', 'col')
- output 3: float32 [10240, 4096], P('row', 'col')
- output 4: float32 [4096], P('row')
- output 5: float32 [10240], P('col')
- output 6: float32 [4096], P('row')
- output 7: float32 [10240], P('col')
- output 8: float32 [10240], P('row')
- output 9: float32 [4096], P('col')
- output 10: bfloat16 [4096, 4096], P(None, 'row')
- output 11: bfloat16 [4096, 10240], P(None, 'row')
All inputs are finite; a program needn't handle non-finite values.
Results may differ from the reference program's by a relative error of at most 0.001.
Values are sent between devices in bfloat16 or wider.
A program may use at most 1 GiB of HBM per device.

```python
import jax
import jax.numpy as jnp
from jax import lax

D_MODEL = 4096
D_FF = 10240
TOKENS = 4096
EPS_ONE = 1e-30
EPS_TWO = 1e-3
TWO_PI = 6.283185307179586


def smooth_field(key, length, log_scale):
    key_amp, key_phase = jax.random.split(key)
    ampl_k = jax.random.normal(key_amp, (3,), jnp.float32)
    phase_k = jax.random.uniform(key_phase, (3,), jnp.float32, minval=0.0, maxval=TWO_PI)
    position = jnp.arange(length, dtype=jnp.float32) / length
    freq_k = jnp.arange(1, 4, dtype=jnp.float32)
    waves = jnp.cos(TWO_PI * position[:, None] * freq_k[None, :] + phase_k[None, :])
    return jnp.exp(log_scale * jnp.sum(waves * ampl_k[None, :], axis=1) / 1.7)


def draw_weight(key, rows, cols):
    key_z, key_r, key_c = jax.random.split(key, 3)
    noise = jax.random.normal(key_z, (rows, cols), jnp.float32)
    row_prof = smooth_field(key_r, rows, 0.5)
    col_prof = smooth_field(key_c, cols, 0.5)
    return noise * (rows ** -0.5) * row_prof[:, None] * col_prof[None, :]


def draw_tokens(key, cols, scale):
    key_z, key_a, key_b = jax.random.split(key, 3)
    noise = jax.random.normal(key_z, (TOKENS, cols), jnp.float32)
    first_half = (jnp.arange(TOKENS) < TOKENS // 2)[:, None]
    profile = jnp.where(first_half, smooth_field(key_a, cols, 0.8)[None, :], smooth_field(key_b, cols, 0.8)[None, :])
    return (noise * profile * scale).astype(jnp.bfloat16)


def draw_stat(key, length):
    return jax.random.uniform(key, (length,), jnp.float32, minval=0.5, maxval=3.0)


def setup_inputs(seed: int = 0) -> dict:
    keys = jax.random.split(jax.random.key(seed), 15)
    tok_scale = TOKENS ** -0.5
    low_end = jnp.array([0.6, 0.6, 0.15], dtype=jnp.float32)
    span_len = jnp.array([0.25, 0.6, 0.15], dtype=jnp.float32)
    unit_draw = jax.random.uniform(keys[14], (3,), jnp.float32)
    return {
        'w_gate': draw_weight(keys[0], D_MODEL, D_FF),
        'w_up': draw_weight(keys[1], D_MODEL, D_FF),
        'w_down': draw_weight(keys[2], D_FF, D_MODEL),
        'x_norm': draw_tokens(keys[3], D_MODEL, tok_scale),
        'x_act': draw_tokens(keys[4], D_FF, tok_scale),
        'dy_gate': draw_tokens(keys[5], D_FF, 1.0),
        'dy_up': draw_tokens(keys[6], D_FF, 1.0),
        'dy_down': draw_tokens(keys[7], D_MODEL, 1.0),
        'r_gate': draw_stat(keys[8], D_MODEL),
        'c_gate': draw_stat(keys[9], D_FF),
        'r_up': draw_stat(keys[10], D_MODEL),
        'c_up': draw_stat(keys[11], D_FF),
        'r_down': draw_stat(keys[12], D_FF),
        'c_down': draw_stat(keys[13], D_MODEL),
        'hyper_params': low_end + span_len * unit_draw,
    }


def factored_step(w_old, grad_w, r_old, c_old, hyper_params):
    beta_two = hyper_params[0]
    grad_sq = grad_w * grad_w + EPS_ONE
    r_new = beta_two * r_old + (1.0 - beta_two) * jnp.mean(grad_sq, axis=1)
    c_new = beta_two * c_old + (1.0 - beta_two) * jnp.mean(grad_sq, axis=0)
    v_est = r_new[:, None] * c_new[None, :] / jnp.mean(r_new)
    update = grad_w * lax.rsqrt(v_est)
    rms_u = jnp.sqrt(jnp.mean(update * update))
    update_hat = update / jnp.maximum(1.0, rms_u / hyper_params[2])
    step_size = hyper_params[1] * jnp.maximum(EPS_TWO, jnp.sqrt(jnp.mean(w_old * w_old)))
    return w_old - step_size * update_hat, r_new, c_new


def weight_grad(activations, grad_out):
    return jnp.dot(activations.T, grad_out, preferred_element_type=jnp.float32)


def input_grad(grad_out, weight):
    return jnp.dot(grad_out, weight.astype(jnp.bfloat16).T, preferred_element_type=jnp.float32)


def reference(w_gate, w_up, w_down, x_norm, x_act, dy_gate, dy_up, dy_down, r_gate, c_gate, r_up, c_up, r_down, c_down, hyper_params):
    new_gate, r_gate_new, c_gate_new = factored_step(w_gate, weight_grad(x_norm, dy_gate), r_gate, c_gate, hyper_params)
    new_up, r_up_new, c_up_new = factored_step(w_up, weight_grad(x_norm, dy_up), r_up, c_up, hyper_params)
    new_down, r_down_new, c_down_new = factored_step(w_down, weight_grad(x_act, dy_down), r_down, c_down, hyper_params)
    dx_norm = (input_grad(dy_gate, w_gate) + input_grad(dy_up, w_up)).astype(jnp.bfloat16)
    dx_act = input_grad(dy_down, w_down).astype(jnp.bfloat16)
    return (new_gate, new_up, new_down, r_gate_new, c_gate_new, r_up_new, c_up_new, r_down_new, c_down_new, dx_norm, dx_act)
```

```python
import jax
import jax.numpy as jnp
from jax import lax
from jax.experimental import pallas as pl
from jax.experimental.pallas import tpu as pltpu
from jax.sharding import PartitionSpec as P

EPS_ONE = 1e-30
EPS_TWO = 1e-3
F32 = jnp.float32
BF16 = jnp.bfloat16
VMEM_LIMIT = 60 * 1024 * 1024
NT = (((1,), (1,)), ((), ()))


def params(*semantics):
    return pltpu.CompilerParams(dimension_semantics=semantics, vmem_limit_bytes=VMEM_LIMIT)


def cost(flops, nbytes):
    return pl.CostEstimate(flops=int(flops), bytes_accessed=int(nbytes), transcendentals=0)


def cast_kernel(w_ref, b_ref, s_ref):
    w = w_ref[...]
    b_ref[...] = w.astype(BF16)

    @pl.when(pl.program_id(0) == 0)
    def _():
        s_ref[...] = jnp.zeros_like(s_ref)

    s_ref[...] += jnp.sum((w * w).reshape(w.shape[0] // 8, 8, w.shape[1]), axis=0)


def cast_weight(w):
    rows, cols = w.shape
    tile = 128
    b, s = pl.pallas_call(
        cast_kernel,
        grid=(rows // tile,),
        in_specs=[pl.BlockSpec((tile, cols), lambda i: (i, 0))],
        out_specs=[pl.BlockSpec((tile, cols), lambda i: (i, 0)), pl.BlockSpec((8, cols), lambda i: (0, 0))],
        out_shape=[jax.ShapeDtypeStruct((rows, cols), BF16), jax.ShapeDtypeStruct((8, cols), F32)],
        compiler_params=params('arbitrary'),
        cost_estimate=cost(w.size * 3, w.size * 6),
        name='cast_weight',
    )(w)
    return b, jnp.sum(s)


def grad_kernel(x_ref, dy_ref, g_ref, row_ref, col_ref, xt_ref):
    step = pl.program_id(0)

    @pl.when(step == 0)
    def _():
        row_ref[...] = jnp.zeros_like(row_ref)
        xt_ref[...] = x_ref[...].T

    g = jnp.dot(xt_ref[...], dy_ref[...], preferred_element_type=F32)
    g_ref[...] = g
    q = g * g + EPS_ONE
    col_ref[...] = jnp.sum(q, axis=0, keepdims=True)
    part = q[:, :128]
    for k in range(1, q.shape[1] // 128):
        part += q[:, k * 128:(k + 1) * 128]
    row_ref[...] += part


def weight_grad(x, dy, tile):
    tokens, m = x.shape
    n = dy.shape[1]
    g, row, col = pl.pallas_call(
        grad_kernel,
        grid=(n // tile,),
        in_specs=[
            pl.BlockSpec((tokens, m), lambda j: (0, 0), pipeline_mode=pl.Buffered(1)),
            pl.BlockSpec((tokens, tile), lambda j: (0, j)),
        ],
        out_specs=[
            pl.BlockSpec((m, tile), lambda j: (0, j)),
            pl.BlockSpec((m, 128), lambda j: (0, 0)),
            pl.BlockSpec((1, tile), lambda j: (0, j)),
        ],
        out_shape=[
            jax.ShapeDtypeStruct((m, n), F32),
            jax.ShapeDtypeStruct((m, 128), F32),
            jax.ShapeDtypeStruct((1, n), F32),
        ],
        scratch_shapes=[pltpu.VMEM((m, tokens), BF16)],
        compiler_params=params('arbitrary'),
        cost_estimate=cost(2 * tokens * m * n, 2 * tokens * (m + n) + 4 * m * n),
        name='weight_grad',
    )(x, dy)
    return g, jnp.sum(row, axis=1), col[0]


def norm_kernel(off_ref, dyg_ref, dyu_ref, wg_ref, wu_ref, out_ref):
    out_ref[...] = lax.dot_general(dyg_ref[...], wg_ref[...], NT, preferred_element_type=F32) + lax.dot_general(
        dyu_ref[...], wu_ref[...], NT, preferred_element_type=F32)


def norm_partial(offset, tokens, dyg, dyu, wg, wu):
    tile = 512
    m, n = wg.shape
    dy_spec = pl.BlockSpec((tile, n), lambda i, off: (off[0] + i, 0))
    w_spec = pl.BlockSpec((m, n), lambda i, off: (0, 0), pipeline_mode=pl.Buffered(1))
    return pl.pallas_call(
        norm_kernel,
        grid_spec=pltpu.PrefetchScalarGridSpec(
            num_scalar_prefetch=1,
            grid=(tokens // tile,),
            in_specs=[dy_spec, dy_spec, w_spec, w_spec],
            out_specs=pl.BlockSpec((tile, m), lambda i, off: (i, 0)),
        ),
        out_shape=jax.ShapeDtypeStruct((tokens, m), F32),
        compiler_params=params('arbitrary'),
        cost_estimate=cost(4 * tokens * m * n, 4 * tokens * n + 4 * m * n + 4 * tokens * m),
        name='norm_partial',
    )((offset // tile).astype(jnp.int32).reshape(1), dyg, dyu, wg, wu)


def act_kernel(dya_ref, dyb_ref, wa_ref, wb_ref, out_ref, acc_ref):
    step = pl.program_id(1)

    @pl.when(step == 0)
    def _():
        acc_ref[...] = lax.dot_general(dya_ref[...], wa_ref[...], NT, preferred_element_type=F32)

    @pl.when(step == 1)
    def _():
        other = lax.dot_general(dyb_ref[...], wb_ref[...], NT, preferred_element_type=F32)
        out_ref[...] = (acc_ref[...] + other).astype(BF16)


def act_grad(dya, dyb, wa, wb):
    tile = 512
    tokens, n = dya.shape
    m = wa.shape[0]
    dy_spec = pl.BlockSpec((tile, n), lambda i, k: (i, 0))
    w_spec = pl.BlockSpec((m, n), lambda i, k: (0, 0), pipeline_mode=pl.Buffered(1))
    return pl.pallas_call(
        act_kernel,
        grid=(tokens // tile, 2),
        in_specs=[dy_spec, dy_spec, w_spec, w_spec],
        out_specs=pl.BlockSpec((tile, m), lambda i, k: (i, 0)),
        out_shape=jax.ShapeDtypeStruct((tokens, m), BF16),
        scratch_shapes=[pltpu.VMEM((tile, m), F32)],
        compiler_params=params('arbitrary', 'arbitrary'),
        cost_estimate=cost(4 * tokens * m * n, 4 * tokens * n + 4 * m * n + 2 * tokens * m),
        name='act_grad',
    )(dya, dyb, wa, wb)


def swap_col(v):
    return lax.ppermute(v, 'col', [(0, 1), (1, 0)])


def sum_row(v, row_size):
    step = 1
    while step < row_size:
        v = v + lax.ppermute(v, 'row', [(i, i ^ step) for i in range(row_size)])
        step *= 2
    return v


def solution(mesh):
    row_size = mesh.shape['row']
    col_size = mesh.shape['col']
    weight_spec = P('row', 'col')
    act_spec = P(None, 'row')
    grad_spec = P(None, 'col')
    in_specs = (weight_spec,) * 3 + (act_spec, act_spec) + (grad_spec,) * 3 + (P('row'), P('col')) * 3 + (P(),)
    out_specs = (weight_spec,) * 3 + (P('row'), P('col')) * 3 + (act_spec, act_spec)

    def body(w_gate, w_up, w_down, x_norm, x_act, dy_gate, dy_up, dy_down, r_gate, c_gate, r_up, c_up, r_down, c_down, hyper_params):
        row = lax.axis_index('row')
        col = lax.axis_index('col')
        tokens = x_norm.shape[0]
        half = tokens // col_size
        beta_two = hyper_params[0]

        share = tokens // row_size
        piece = swap_col(lax.dynamic_slice_in_dim(dy_down, row * share, share, axis=0))
        dy_down_other = lax.all_gather(piece, 'row', axis=0, tiled=True)

        b_gate, w_sq_gate = cast_weight(w_gate)
        b_up, w_sq_up = cast_weight(w_up)
        sent = norm_partial((1 - col) * half, half, dy_gate, dy_up, b_gate, b_up)
        got = swap_col(sent)

        b_down, w_sq_down = cast_weight(w_down)
        cut = 768
        b_down_other = [swap_col(b_down[:cut]), swap_col(b_down[cut:])]

        own = norm_partial(col * half, half, dy_gate, dy_up, b_gate, b_up)
        g_gate, row_gate, col_gate = weight_grad(x_norm, dy_gate, 512)
        g_up, row_up, col_up = weight_grad(x_norm, dy_up, 512)
        g_down, row_down, col_down = weight_grad(x_act, dy_down, 256)

        mine = (own + got).astype(BF16)
        theirs = swap_col(mine)
        dx_norm = jnp.where(col == 0, jnp.concatenate([mine, theirs]), jnp.concatenate([theirs, mine]))

        sizes_r = [r_gate.shape[0], r_up.shape[0], r_down.shape[0]]
        sizes_c = [c_gate.shape[0], c_up.shape[0], c_down.shape[0]]
        totals = [(sizes_r[k] * row_size, sizes_c[k] * col_size) for k in range(3)]
        row_all = jnp.concatenate([row_gate, row_up, row_down])
        row_all = row_all + swap_col(row_all)
        row_sums = jnp.split(row_all, [sizes_r[0], sizes_r[0] + sizes_r[1]])
        r_old = [r_gate, r_up, r_down]
        c_old = [c_gate, c_up, c_down]
        r_new = [beta_two * r_old[k] + (1.0 - beta_two) * (row_sums[k] / totals[k][1]) for k in range(3)]
        r_part = jnp.zeros((128,), F32).at[:3].set(jnp.stack([jnp.sum(r) for r in r_new]))
        col_all = sum_row(jnp.concatenate([col_gate, col_up, col_down, r_part]), row_size)
        offs = [0, sizes_c[0], sizes_c[0] + sizes_c[1], sum(sizes_c)]
        c_new = [
            beta_two * c_old[k] + (1.0 - beta_two) * (col_all[offs[k]:offs[k + 1]] / totals[k][0]) for k in range(3)
        ]
        r_mean = [col_all[offs[3] + k] / totals[k][0] for k in range(3)]
        grads = [g_gate, g_up, g_down]
        updates = [grads[k] * lax.rsqrt(r_new[k][:, None] * c_new[k][None, :] / r_mean[k]) for k in range(3)]
        scalars = jnp.stack([jnp.sum(u * u) for u in updates] + [w_sq_gate, w_sq_up, w_sq_down])
        scalars = sum_row(jnp.zeros((128,), F32).at[:6].set(scalars), row_size)
        scalars = scalars + swap_col(scalars)
        weights = [w_gate, w_up, w_down]
        new = []
        for k in range(3):
            size = totals[k][0] * totals[k][1]
            rms_u = jnp.sqrt(scalars[k] / size)
            step_size = hyper_params[1] * jnp.maximum(EPS_TWO, jnp.sqrt(scalars[3 + k] / size))
            new.append(weights[k] - step_size * (updates[k] / jnp.maximum(1.0, rms_u / hyper_params[2])))

        dx_act = jnp.concatenate(
            [
                act_grad(dy_down, dy_down_other, b_down[:cut], b_down_other[0]),
                act_grad(dy_down, dy_down_other, b_down[cut:], b_down_other[1]),
            ],
            axis=1,
        )
        return (*new, r_new[0], c_new[0], r_new[1], c_new[1], r_new[2], c_new[2], dx_norm, dx_act)

    return jax.shard_map(body, mesh=mesh, in_specs=in_specs, out_specs=out_specs, check_vma=False)
```

```python
import functools

import jax
import jax.numpy as jnp
from jax import lax
from jax.experimental import pallas as pl
from jax.experimental.pallas import tpu as pltpu
from jax.sharding import PartitionSpec as P

EPS_ONE = 1e-30
EPS_TWO = 1e-3
F32 = jnp.float32
BF16 = jnp.bfloat16
VMEM_LIMIT = 60 * 1024 * 1024
NT = (((1,), (1,)), ((), ()))


def params(*semantics):
    return pltpu.CompilerParams(dimension_semantics=semantics, vmem_limit_bytes=VMEM_LIMIT)


def cost(flops, nbytes):
    return pl.CostEstimate(flops=int(flops), bytes_accessed=int(nbytes), transcendentals=0)


def fold_squares(v):
    return jnp.sum((v * v).reshape(v.shape[0] // 8, 8, v.shape[1]), axis=0)


def cast_kernel(first, w_ref, a_ref, b_ref, s_ref):
    step = pl.program_id(0)
    w = w_ref[...]

    @pl.when(step < first)
    def _():
        a_ref[...] = w.astype(BF16)

    @pl.when(step >= first)
    def _():
        b_ref[...] = w.astype(BF16)

    @pl.when(step == 0)
    def _():
        s_ref[...] = jnp.zeros_like(s_ref)

    s_ref[...] += fold_squares(w)


def cast_weight(w, cut):
    rows, cols = w.shape
    tile = 256
    first = cut // tile
    a, b, s = pl.pallas_call(
        functools.partial(cast_kernel, first),
        grid=(rows // tile,),
        in_specs=[pl.BlockSpec((tile, cols), lambda i: (i, 0))],
        out_specs=[
            pl.BlockSpec((tile, cols), lambda i: (jnp.minimum(i, first - 1), 0)),
            pl.BlockSpec((tile, cols), lambda i: (jnp.maximum(i - first, 0), 0)),
            pl.BlockSpec((8, cols), lambda i: (0, 0)),
        ],
        out_shape=[
            jax.ShapeDtypeStruct((cut, cols), BF16),
            jax.ShapeDtypeStruct((rows - cut, cols), BF16),
            jax.ShapeDtypeStruct((8, cols), F32),
        ],
        compiler_params=params('arbitrary'),
        cost_estimate=cost(w.size * 1000, w.size * 6),
        name='cast_weight',
    )(w)
    return a, b, jnp.sum(s)


def grad_block(xt_ref, dy_ref, g_ref, row_ref, col_ref):
    g = jnp.dot(xt_ref[...], dy_ref[...], preferred_element_type=F32)
    g_ref[...] = g
    q = g * g + EPS_ONE
    col_ref[...] = jnp.sum(q, axis=0, keepdims=True)
    part = q[:, :128]
    for k in range(1, q.shape[1] // 128):
        part += q[:, k * 128:(k + 1) * 128]
    row_ref[...] += part


def grad_kernel(count, steps, x_ref, *refs):
    dy, out, xt_ref = refs[:count], refs[count:-1], refs[-1]
    step = pl.program_id(0)

    @pl.when(step == 0)
    def _():
        for k in range(count):
            out[3 * k + 1][...] = jnp.zeros_like(out[3 * k + 1])
        xt_ref[...] = x_ref[...].T

    for k in range(count):
        @pl.when((step >= k * steps) & (step < (k + 1) * steps))
        def _():
            grad_block(xt_ref, dy[k], *out[3 * k:3 * k + 3])


def weight_grads(x, dys, tile):
    tokens, m = x.shape
    n = dys[0].shape[1]
    steps = n // tile
    count = len(dys)

    def block(k):
        return lambda j: (0, jnp.clip(j - k * steps, 0, steps - 1))

    out_specs, out_shape = [], []
    for k in range(count):
        out_specs += [
            pl.BlockSpec((m, tile), block(k)),
            pl.BlockSpec((m, 128), lambda j: (0, 0)),
            pl.BlockSpec((1, tile), block(k)),
        ]
        out_shape += [
            jax.ShapeDtypeStruct((m, n), F32),
            jax.ShapeDtypeStruct((m, 128), F32),
            jax.ShapeDtypeStruct((1, n), F32),
        ]
    out = pl.pallas_call(
        functools.partial(grad_kernel, count, steps),
        grid=(steps * count,),
        in_specs=[pl.BlockSpec((tokens, m), lambda j: (0, 0), pipeline_mode=pl.Buffered(1))]
        + [pl.BlockSpec((tokens, tile), block(k)) for k in range(count)],
        out_specs=out_specs,
        out_shape=out_shape,
        scratch_shapes=[pltpu.VMEM((m, tokens), BF16)],
        compiler_params=params('arbitrary'),
        cost_estimate=cost(2 * count * tokens * m * n, count * (2 * tokens * (m + n) + 4 * m * n)),
        name='weight_grads',
    )(x, *dys)
    return [(out[3 * k], jnp.sum(out[3 * k + 1], axis=1), out[3 * k + 2][0]) for k in range(count)]


def norm_kernel(steps, squares, off_ref, dyg_ref, dyu_ref, wg_ref, wu_ref, *out):
    step = pl.program_id(0)

    def add(dy_ref, w_ref, k):
        w = w_ref[...]
        b = w.astype(BF16)
        half = dy_ref.shape[0] // 2
        for i in range(2):
            part = lax.dot_general(dy_ref[i * half:(i + 1) * half, :], b, NT, preferred_element_type=F32)
            out[i][...] += part
        if squares:
            out[2 + k][...] += fold_squares(w)

    @pl.when(step == 0)
    def _():
        for ref in out:
            ref[...] = jnp.zeros_like(ref)

    @pl.when(step < steps)
    def _():
        add(dyg_ref, wg_ref, 0)

    @pl.when(step >= steps)
    def _():
        add(dyu_ref, wu_ref, 1)


def norm_partial(offset, tokens, dyg, dyu, wg, wu, squares):
    tile = 1024
    m, n = wg.shape
    steps = n // tile

    def block(row, k):
        return lambda j, off: (off[0] if row else 0, jnp.clip(j - k * steps, 0, steps - 1))

    out_specs = [pl.BlockSpec((tokens // 2, m), lambda j, off: (0, 0))] * 2
    out_shape = [jax.ShapeDtypeStruct((tokens // 2, m), F32)] * 2
    if squares:
        out_specs += [pl.BlockSpec((8, tile), lambda j, off: (0, 0))] * 2
        out_shape += [jax.ShapeDtypeStruct((8, tile), F32)] * 2
    out = pl.pallas_call(
        functools.partial(norm_kernel, steps, squares),
        grid_spec=pltpu.PrefetchScalarGridSpec(
            num_scalar_prefetch=1,
            grid=(2 * steps,),
            in_specs=[
                pl.BlockSpec((tokens, tile), block(True, 0)),
                pl.BlockSpec((tokens, tile), block(True, 1)),
                pl.BlockSpec((m, tile), block(False, 0)),
                pl.BlockSpec((m, tile), block(False, 1)),
            ],
            out_specs=out_specs,
        ),
        out_shape=out_shape,
        compiler_params=params('arbitrary'),
        cost_estimate=cost(4 * tokens * m * n, 4 * tokens * n + 8 * m * n + 4 * tokens * m),
        name='norm_partial',
    )((offset // tokens).astype(jnp.int32).reshape(1), dyg, dyu, wg, wu)
    return [*out[:2], *[jnp.sum(s) for s in out[2:]]]


def act_kernel(block, parts, dya_ref, dyb_ref, *refs):
    out_ref, acc_ref = refs[-2:]
    done = 0
    for wa_ref, wb_ref in zip(refs[:parts], refs[parts:2 * parts]):
        count = wa_ref.shape[0] // block

        @pl.loop(0, count)
        def _(k):
            rows = pl.ds(pl.multiple_of(k * block, block), block)
            acc_ref[k] = lax.dot_general(dya_ref[...], wa_ref[rows, :], NT, preferred_element_type=F32)

        @pl.loop(0, count)
        def _(k):
            rows = pl.ds(pl.multiple_of(k * block, block), block)
            cols = pl.ds(pl.multiple_of(done + k * block, block), block)
            other = lax.dot_general(dyb_ref[...], wb_ref[rows, :], NT, preferred_element_type=F32)
            out_ref[:, cols] = (acc_ref[k] + other).astype(BF16)

        done += wa_ref.shape[0]


def act_grad(dya, dyb, wa, wb):
    tile, block = 512, 256
    tokens, n = dya.shape
    m = sum(w.shape[0] for w in wa)
    dy_spec = pl.BlockSpec((tile, n), lambda i: (i, 0))
    w_specs = [pl.BlockSpec(w.shape, lambda i: (0, 0), pipeline_mode=pl.Buffered(1)) for w in (*wa, *wb)]
    return pl.pallas_call(
        functools.partial(act_kernel, block, len(wa)),
        grid=(tokens // tile,),
        in_specs=[dy_spec, dy_spec, *w_specs],
        out_specs=pl.BlockSpec((tile, m), lambda i: (i, 0)),
        out_shape=jax.ShapeDtypeStruct((tokens, m), BF16),
        scratch_shapes=[pltpu.VMEM((max(w.shape[0] for w in wa) // block, tile, block), F32)],
        compiler_params=params('arbitrary'),
        cost_estimate=cost(4 * tokens * m * n, 4 * tokens * n + 4 * m * n + 2 * tokens * m),
        name='act_grad',
    )(dya, dyb, *wa, *wb)


def swap_col(v):
    return lax.ppermute(v, 'col', [(0, 1), (1, 0)])


def sum_row(v, row_size):
    step = 1
    while step < row_size:
        v = v + lax.ppermute(v, 'row', [(i, i ^ step) for i in range(row_size)])
        step *= 2
    return v


def solution(mesh):
    row_size = mesh.shape['row']
    col_size = mesh.shape['col']
    weight_spec = P('row', 'col')
    act_spec = P(None, 'row')
    grad_spec = P(None, 'col')
    in_specs = (weight_spec,) * 3 + (act_spec, act_spec) + (grad_spec,) * 3 + (P('row'), P('col')) * 3 + (P(),)
    out_specs = (weight_spec,) * 3 + (P('row'), P('col')) * 3 + (act_spec, act_spec)

    def body(w_gate, w_up, w_down, x_norm, x_act, dy_gate, dy_up, dy_down, r_gate, c_gate, r_up, c_up, r_down, c_down, hyper_params):
        row = lax.axis_index('row')
        col = lax.axis_index('col')
        tokens = x_norm.shape[0]
        half = tokens // col_size
        beta_two = hyper_params[0]

        share = tokens // row_size
        piece = lax.dynamic_slice_in_dim(dy_down, row * share, share, axis=0)
        piece = swap_col(piece)
        dy_down_other = lax.all_gather(piece, 'row', axis=0, tiled=True)
        b_down_a, b_down_b, w_sq_down = cast_weight(w_down, 768)
        o_down_a = swap_col(b_down_a)

        (g_gate, row_gate, col_gate), (g_up, row_up, col_up) = weight_grads(x_norm, [dy_gate, dy_up], 512)
        ((g_down, row_down, col_down),) = weight_grads(x_act, [dy_down], 256)
        row_all = jnp.concatenate([row_gate, row_up, row_down])
        row_peer = swap_col(row_all)
        o_down_b = swap_col(b_down_b)
        sent = norm_partial((1 - col) * half, half, dy_gate, dy_up, w_gate, w_up, False)
        got0 = swap_col(sent[0])
        own0, own1, w_sq_gate, w_sq_up = norm_partial(col * half, half, dy_gate, dy_up, w_gate, w_up, True)

        sizes_r = [r_gate.shape[0], r_up.shape[0], r_down.shape[0]]
        sizes_c = [c_gate.shape[0], c_up.shape[0], c_down.shape[0]]
        totals = [(sizes_r[k] * row_size, sizes_c[k] * col_size) for k in range(3)]
        row_all = row_all + row_peer
        row_sums = jnp.split(row_all, [sizes_r[0], sizes_r[0] + sizes_r[1]])
        r_old = [r_gate, r_up, r_down]
        c_old = [c_gate, c_up, c_down]
        r_new = [beta_two * r_old[k] + (1.0 - beta_two) * (row_sums[k] / totals[k][1]) for k in range(3)]
        r_part = jnp.zeros((128,), F32).at[:3].set(jnp.stack([jnp.sum(r) for r in r_new]))
        col_all = sum_row(jnp.concatenate([col_gate, col_up, col_down, r_part]), row_size)
        offs = [0, sizes_c[0], sizes_c[0] + sizes_c[1], sum(sizes_c)]
        c_new = [
            beta_two * c_old[k] + (1.0 - beta_two) * (col_all[offs[k]:offs[k + 1]] / totals[k][0]) for k in range(3)
        ]
        r_mean = [col_all[offs[3] + k] / totals[k][0] for k in range(3)]
        grads = [g_gate, g_up, g_down]
        updates = [grads[k] * lax.rsqrt(r_new[k][:, None] * c_new[k][None, :] / r_mean[k]) for k in range(3)]
        scalars = jnp.stack([jnp.sum(u * u) for u in updates] + [w_sq_gate, w_sq_up, w_sq_down])
        scalars = sum_row(jnp.zeros((128,), F32).at[:6].set(scalars), row_size)
        scalars_peer = swap_col(scalars)
        got1 = swap_col(sent[1])
        dx_act = act_grad(dy_down, dy_down_other, [b_down_a, b_down_b], [o_down_a, o_down_b])
        scalars = scalars + scalars_peer
        weights = [w_gate, w_up, w_down]
        new = []
        for k in range(3):
            size = totals[k][0] * totals[k][1]
            rms_u = jnp.sqrt(scalars[k] / size)
            step_size = hyper_params[1] * jnp.maximum(EPS_TWO, jnp.sqrt(scalars[3 + k] / size))
            new.append(weights[k] - step_size * (updates[k] / jnp.maximum(1.0, rms_u / hyper_params[2])))

        mine0 = (own0 + got0).astype(BF16)
        theirs0 = swap_col(mine0)
        mine1 = (own1 + got1).astype(BF16)
        theirs1 = swap_col(mine1)
        dx_norm = jnp.where(
            col == 0,
            jnp.concatenate([mine0, mine1, theirs0, theirs1]),
            jnp.concatenate([theirs0, theirs1, mine0, mine1]),
        )
        return (*new, r_new[0], c_new[0], r_new[1], c_new[1], r_new[2], c_new[2], dx_norm, dx_act)

    return jax.shard_map(body, mesh=mesh, in_specs=in_specs, out_specs=out_specs, check_vma=False)
```

```python
import functools

import jax
import jax.numpy as jnp
from jax import lax
from jax.experimental import pallas as pl
from jax.experimental.pallas import tpu as pltpu
from jax.sharding import PartitionSpec as P

EPS_ONE = 1e-30
EPS_TWO = 1e-3
F32 = jnp.float32
BF16 = jnp.bfloat16
VMEM_LIMIT = 60 * 1024 * 1024
NT = (((1,), (1,)), ((), ()))


def params(*semantics):
    return pltpu.CompilerParams(dimension_semantics=semantics, vmem_limit_bytes=VMEM_LIMIT)


def cost(flops, nbytes):
    return pl.CostEstimate(flops=int(flops), bytes_accessed=int(nbytes), transcendentals=0)


def fold_squares(v):
    return jnp.sum((v * v).reshape(v.shape[0] // 8, 8, v.shape[1]), axis=0)


def cast_kernel(first, w_ref, a_ref, b_ref, s_ref):
    step = pl.program_id(0)
    w = w_ref[...]

    @pl.when(step < first)
    def _():
        a_ref[...] = w.astype(BF16)

    @pl.when(step >= first)
    def _():
        b_ref[...] = w.astype(BF16)

    @pl.when(step == 0)
    def _():
        s_ref[...] = jnp.zeros_like(s_ref)

    s_ref[...] += fold_squares(w)


def cast_weight(w, cut):
    rows, cols = w.shape
    tile = 256
    first = cut // tile
    a, b, s = pl.pallas_call(
        functools.partial(cast_kernel, first),
        grid=(rows // tile,),
        in_specs=[pl.BlockSpec((tile, cols), lambda i: (i, 0))],
        out_specs=[
            pl.BlockSpec((tile, cols), lambda i: (jnp.minimum(i, first - 1), 0)),
            pl.BlockSpec((tile, cols), lambda i: (jnp.maximum(i - first, 0), 0)),
            pl.BlockSpec((8, cols), lambda i: (0, 0)),
        ],
        out_shape=[
            jax.ShapeDtypeStruct((cut, cols), BF16),
            jax.ShapeDtypeStruct((rows - cut, cols), BF16),
            jax.ShapeDtypeStruct((8, cols), F32),
        ],
        compiler_params=params('arbitrary'),
        cost_estimate=cost(w.size * 1000, w.size * 6),
        name='cast_weight',
    )(w)
    return a, b, jnp.sum(s)


def grad_block(xt_ref, dy_ref, g_ref, row_ref, col_ref):
    g = jnp.dot(xt_ref[...], dy_ref[...], preferred_element_type=F32)
    g_ref[...] = g
    q = g * g + EPS_ONE
    col_ref[...] = jnp.sum(q, axis=0, keepdims=True)
    part = q[:, :128]
    for k in range(1, q.shape[1] // 128):
        part += q[:, k * 128:(k + 1) * 128]
    row_ref[...] += part


def grad_kernel(count, steps, x_ref, *refs):
    dy, out, xt_ref = refs[:count], refs[count:-1], refs[-1]
    step = pl.program_id(0)

    @pl.when(step == 0)
    def _():
        for k in range(count):
            out[3 * k + 1][...] = jnp.zeros_like(out[3 * k + 1])
        xt_ref[...] = x_ref[...].T

    for k in range(count):
        @pl.when((step >= k * steps) & (step < (k + 1) * steps))
        def _():
            grad_block(xt_ref, dy[k], *out[3 * k:3 * k + 3])


def weight_grads(x, dys, tile):
    tokens, m = x.shape
    n = dys[0].shape[1]
    steps = n // tile
    count = len(dys)

    def block(k):
        return lambda j: (0, jnp.clip(j - k * steps, 0, steps - 1))

    out_specs, out_shape = [], []
    for k in range(count):
        out_specs += [
            pl.BlockSpec((m, tile), block(k)),
            pl.BlockSpec((m, 128), lambda j: (0, 0)),
            pl.BlockSpec((1, tile), block(k)),
        ]
        out_shape += [
            jax.ShapeDtypeStruct((m, n), F32),
            jax.ShapeDtypeStruct((m, 128), F32),
            jax.ShapeDtypeStruct((1, n), F32),
        ]
    out = pl.pallas_call(
        functools.partial(grad_kernel, count, steps),
        grid=(steps * count,),
        in_specs=[pl.BlockSpec((tokens, m), lambda j: (0, 0), pipeline_mode=pl.Buffered(1))]
        + [pl.BlockSpec((tokens, tile), block(k)) for k in range(count)],
        out_specs=out_specs,
        out_shape=out_shape,
        scratch_shapes=[pltpu.VMEM((m, tokens), BF16)],
        compiler_params=params('arbitrary'),
        cost_estimate=cost(2 * count * tokens * m * n, count * (2 * tokens * (m + n) + 4 * m * n)),
        name='weight_grads',
    )(x, *dys)
    return [(out[3 * k], jnp.sum(out[3 * k + 1], axis=1), out[3 * k + 2][0]) for k in range(count)]


def norm_kernel(chunk, start_ref, dyg_ref, dyu_ref, wg_ref, wu_ref, *refs):
    out, squares, (acc_ref, wb_ref, stage_ref, sems) = refs[:4], refs[4:6], refs[6:]
    step = pl.program_id(0)
    weights = (wg_ref, wu_ref)
    chunks = wg_ref.shape[1] // chunk
    slots = stage_ref.shape[0]
    per_out = pl.num_programs(0) // 4

    def fetch(matrix, c):
        slot = lax.rem(matrix * chunks + c, slots)
        cols = pl.ds(pl.multiple_of(c * chunk, chunk), chunk)
        return pltpu.make_async_copy(weights[matrix].at[:, cols], stage_ref.at[slot], sems.at[slot])

    @pl.when(step == 0)
    def _():
        for c in range(slots):
            fetch(0, c).start()
        acc_ref[...] = jnp.zeros_like(acc_ref)
        for k, dy_ref in enumerate((dyg_ref, dyu_ref)):
            squares[k][...] = jnp.zeros_like(squares[k])

            @pl.loop(0, chunks)
            def _(c):
                fetch(k, c).wait()
                slot = lax.rem(k * chunks + c, slots)
                cols = pl.ds(pl.multiple_of(c * chunk, chunk), chunk)
                w = stage_ref[slot]
                wb_ref[k, :, cols] = w.astype(BF16)
                squares[k][...] += fold_squares(w)

                @pl.when(c + slots < chunks)
                def _():
                    fetch(k, c + slots).start()

                if k == 0:
                    @pl.when(c + slots >= chunks)
                    def _():
                        fetch(1, c + slots - chunks).start()

                acc_ref[...] += lax.dot_general(dy_ref[:, cols], wb_ref[k, :, cols], NT, preferred_element_type=F32)

    @pl.when(step > 0)
    def _():
        acc_ref[...] = lax.dot_general(dyg_ref[...], wb_ref[0], NT, preferred_element_type=F32) + lax.dot_general(
            dyu_ref[...], wb_ref[1], NT, preferred_element_type=F32)

    for k in range(4):
        @pl.when((step >= k * per_out) & (step < (k + 1) * per_out))
        def _():
            out[k][...] = acc_ref[...]


def norm_partial(first, dyg, dyu, wg, wu):
    tile, chunk, slots = 512, 1024, 3
    tokens, n = dyg.shape
    m = wg.shape[0]
    tiles = tokens // tile
    per_out = tiles // 4
    dy_spec = pl.BlockSpec((tile, n), lambda i, start: (lax.rem(i + start[0], tiles), 0))
    any_spec = pl.BlockSpec(memory_space=pl.ANY)

    def block(k):
        return lambda i, start: (jnp.clip(i - k * per_out, 0, per_out - 1), 0)

    out = pl.pallas_call(
        functools.partial(norm_kernel, chunk),
        grid_spec=pltpu.PrefetchScalarGridSpec(
            num_scalar_prefetch=1,
            grid=(tiles,),
            in_specs=[dy_spec, dy_spec, any_spec, any_spec],
            out_specs=[pl.BlockSpec((tile, m), block(k)) for k in range(4)]
            + [pl.BlockSpec((8, chunk), lambda i, start: (0, 0))] * 2,
            scratch_shapes=[
                pltpu.VMEM((tile, m), F32),
                pltpu.VMEM((2, m, n), BF16),
                pltpu.VMEM((slots, m, chunk), F32),
                pltpu.SemaphoreType.DMA((slots,)),
            ],
        ),
        out_shape=[jax.ShapeDtypeStruct((tokens // 4, m), F32)] * 4 + [jax.ShapeDtypeStruct((8, chunk), F32)] * 2,
        compiler_params=params('arbitrary'),
        cost_estimate=cost(4 * tokens * m * n, 4 * tokens * n + 8 * m * n + 4 * tokens * m),
        name='norm_partial',
    )((first * (tiles // 2)).astype(jnp.int32).reshape(1), dyg, dyu, wg, wu)
    return [*out[:4], *[jnp.sum(v) for v in out[4:]]]


def act_kernel(parts, dya_ref, dyb_ref, *refs):
    out_ref, acc_ref = refs[-2:]

    def halves(dy_ref, w_refs):
        done = 0
        for w_ref in w_refs:
            yield slice(done, done + w_ref.shape[0]), lax.dot_general(
                dy_ref[...], w_ref[...], NT, preferred_element_type=F32)
            done += w_ref.shape[0]

    @pl.when(pl.program_id(0) >= 0)
    def _():
        for cols, part in halves(dya_ref, refs[:parts]):
            acc_ref[:, cols] = part

    @pl.when(pl.program_id(0) < pl.num_programs(0))
    def _():
        for cols, part in halves(dyb_ref, refs[parts:2 * parts]):
            out_ref[:, cols] = (acc_ref[:, cols] + part).astype(BF16)


def act_grad(dya, dyb, wa, wb):
    tile = 512
    tokens, n = dya.shape
    m = sum(w.shape[0] for w in wa)
    dy_spec = pl.BlockSpec((tile, n), lambda i: (i, 0))
    w_specs = [pl.BlockSpec(w.shape, lambda i: (0, 0), pipeline_mode=pl.Buffered(1)) for w in (*wa, *wb)]
    return pl.pallas_call(
        functools.partial(act_kernel, len(wa)),
        grid=(tokens // tile,),
        in_specs=[dy_spec, dy_spec, *w_specs],
        out_specs=pl.BlockSpec((tile, m), lambda i: (i, 0)),
        out_shape=jax.ShapeDtypeStruct((tokens, m), BF16),
        scratch_shapes=[pltpu.VMEM((tile, m), F32)],
        compiler_params=params('arbitrary'),
        cost_estimate=cost(4 * tokens * m * n, 4 * tokens * n + 4 * m * n + 2 * tokens * m),
        name='act_grad',
    )(dya, dyb, *wa, *wb)


def lanes(values):
    index = lax.iota(jnp.int32, 128)
    return sum(jnp.where(index == k, v, 0.0) for k, v in enumerate(values))


def swap_col(v):
    return lax.ppermute(v, 'col', [(0, 1), (1, 0)])


def sum_row(v, row_size):
    step = 1
    while step < row_size:
        v = v + lax.ppermute(v, 'row', [(i, i ^ step) for i in range(row_size)])
        step *= 2
    return v


def solution(mesh):
    row_size = mesh.shape['row']
    col_size = mesh.shape['col']
    weight_spec = P('row', 'col')
    act_spec = P(None, 'row')
    grad_spec = P(None, 'col')
    in_specs = (weight_spec,) * 3 + (act_spec, act_spec) + (grad_spec,) * 3 + (P('row'), P('col')) * 3 + (P(),)
    out_specs = (weight_spec,) * 3 + (P('row'), P('col')) * 3 + (act_spec, act_spec)

    def body(w_gate, w_up, w_down, x_norm, x_act, dy_gate, dy_up, dy_down, r_gate, c_gate, r_up, c_up, r_down, c_down, hyper_params):
        row = lax.axis_index('row')
        col = lax.axis_index('col')
        tokens = x_norm.shape[0]
        half = tokens // col_size
        beta_two = hyper_params[0]

        share = tokens // row_size
        piece = lax.dynamic_slice_in_dim(dy_down, row * share, share, axis=0)
        piece = swap_col(piece)
        dy_down_other = lax.all_gather(piece, 'row', axis=0, tiled=True)
        b_down_a, b_down_b, w_sq_down = cast_weight(w_down, 768)
        o_down_a = swap_col(b_down_a)

        (g_gate, row_gate, col_gate), (g_up, row_up, col_up) = weight_grads(x_norm, [dy_gate, dy_up], 512)
        ((g_down, row_down, col_down),) = weight_grads(x_act, [dy_down], 256)
        row_all = jnp.concatenate([row_gate, row_up, row_down])
        row_peer = swap_col(row_all)
        o_down_b = swap_col(b_down_b)
        sent0, sent1, own0, own1, w_sq_gate, w_sq_up = norm_partial(1 - col, dy_gate, dy_up, w_gate, w_up)
        got0 = swap_col(sent0)

        sizes_r = [r_gate.shape[0], r_up.shape[0], r_down.shape[0]]
        sizes_c = [c_gate.shape[0], c_up.shape[0], c_down.shape[0]]
        totals = [(sizes_r[k] * row_size, sizes_c[k] * col_size) for k in range(3)]
        row_all = row_all + row_peer
        row_sums = jnp.split(row_all, [sizes_r[0], sizes_r[0] + sizes_r[1]])
        r_old = [r_gate, r_up, r_down]
        c_old = [c_gate, c_up, c_down]
        r_new = [beta_two * r_old[k] + (1.0 - beta_two) * (row_sums[k] / totals[k][1]) for k in range(3)]
        r_part = lanes([jnp.sum(r) for r in r_new])
        col_all = sum_row(jnp.concatenate([col_gate, col_up, col_down, r_part]), row_size)
        offs = [0, sizes_c[0], sizes_c[0] + sizes_c[1], sum(sizes_c)]
        c_new = [
            beta_two * c_old[k] + (1.0 - beta_two) * (col_all[offs[k]:offs[k + 1]] / totals[k][0]) for k in range(3)
        ]
        r_mean = [col_all[offs[3] + k:offs[3] + k + 1] / totals[k][0] for k in range(3)]
        grads = [g_gate, g_up, g_down]
        updates = [grads[k] * lax.rsqrt((r_new[k] / r_mean[k])[:, None] * c_new[k][None, :]) for k in range(3)]
        scalars = lanes([jnp.sum(u * u) for u in updates] + [w_sq_gate, w_sq_up, w_sq_down])
        scalars = sum_row(scalars, row_size)
        scalars_peer = swap_col(scalars)
        got1 = swap_col(sent1)
        dx_act = act_grad(dy_down, dy_down_other, [b_down_a, b_down_b], [o_down_a, o_down_b])
        scalars = scalars + scalars_peer
        size = float(totals[0][0] * totals[0][1])
        rms_u = jnp.sqrt(scalars[:3] / size)
        rms_w = jnp.sqrt(scalars[3:6] / size)
        scale = hyper_params[1:2] * jnp.maximum(EPS_TWO, rms_w) / jnp.maximum(1.0, rms_u / hyper_params[2:3])
        weights = [w_gate, w_up, w_down]
        new = [weights[k] - scale[k:k + 1, None] * updates[k] for k in range(3)]

        mine0 = (own0 + got0).astype(BF16)
        theirs0 = swap_col(mine0)
        mine1 = (own1 + got1).astype(BF16)
        theirs1 = swap_col(mine1)
        dx_norm = jnp.where(
            col == 0,
            jnp.concatenate([mine0, mine1, theirs0, theirs0]),
            jnp.concatenate([theirs0, theirs0, mine0, mine1]),
        )
        dx_norm = lax.dynamic_update_slice_in_dim(dx_norm, theirs1, (1 - col) * half + half // 2, axis=0)
        return (*new, r_new[0], c_new[0], r_new[1], c_new[1], r_new[2], c_new[2], dx_norm, dx_act)

    return jax.shard_map(body, mesh=mesh, in_specs=in_specs, out_specs=out_specs, check_vma=False)
```

```python
import functools

import jax
import jax.numpy as jnp
from jax import lax
from jax.experimental import pallas as pl
from jax.experimental.pallas import tpu as pltpu
from jax.sharding import PartitionSpec as P

EPS_ONE = 1e-30
EPS_TWO = 1e-3
F32 = jnp.float32
BF16 = jnp.bfloat16
VMEM_LIMIT = 60 * 1024 * 1024
NT = (((1,), (1,)), ((), ()))


def params(*semantics):
    return pltpu.CompilerParams(dimension_semantics=semantics, vmem_limit_bytes=VMEM_LIMIT)


def cost(flops, nbytes):
    return pl.CostEstimate(flops=int(flops), bytes_accessed=int(nbytes), transcendentals=0)


def fold_squares(v):
    return jnp.sum((v * v).reshape(v.shape[0] // 8, 8, v.shape[1]), axis=0)


def cast_kernel(first, w_ref, a_ref, b_ref, s_ref):
    step = pl.program_id(0)
    w = w_ref[...]

    @pl.when(step < first)
    def _():
        a_ref[...] = w.astype(BF16)

    @pl.when(step >= first)
    def _():
        b_ref[...] = w.astype(BF16)

    @pl.when(step == 0)
    def _():
        s_ref[...] = jnp.zeros_like(s_ref)

    s_ref[...] += fold_squares(w)


def cast_weight(w, cut):
    rows, cols = w.shape
    tile = 256
    first = cut // tile
    a, b, s = pl.pallas_call(
        functools.partial(cast_kernel, first),
        grid=(rows // tile,),
        in_specs=[pl.BlockSpec((tile, cols), lambda i: (i, 0))],
        out_specs=[
            pl.BlockSpec((tile, cols), lambda i: (jnp.minimum(i, first - 1), 0)),
            pl.BlockSpec((tile, cols), lambda i: (jnp.maximum(i - first, 0), 0)),
            pl.BlockSpec((8, cols), lambda i: (0, 0)),
        ],
        out_shape=[
            jax.ShapeDtypeStruct((cut, cols), BF16),
            jax.ShapeDtypeStruct((rows - cut, cols), BF16),
            jax.ShapeDtypeStruct((8, cols), F32),
        ],
        compiler_params=params('arbitrary'),
        cost_estimate=cost(w.size * 1000, w.size * 6),
        name='cast_weight',
    )(w)
    return a, b, s


def grad_block(xt_ref, dy_ref, g_ref, row_ref, col_ref):
    g = jnp.dot(xt_ref[...], dy_ref[...], preferred_element_type=F32)
    g_ref[...] = g
    q = g * g + EPS_ONE
    col_ref[...] = jnp.sum(q, axis=0, keepdims=True)
    part = q[:, :128]
    for k in range(1, q.shape[1] // 128):
        part += q[:, k * 128:(k + 1) * 128]
    row_ref[...] += part


def grad_kernel(count, steps, x_ref, *refs):
    dy, out, xt_ref, part_ref = refs[:count], refs[count:-2], refs[-2], refs[-1]
    step = pl.program_id(0)

    @pl.when(step == 0)
    def _():
        xt_ref[...] = x_ref[...].T

    for k in range(count):
        @pl.when(step == k * steps)
        def _():
            part_ref[...] = jnp.zeros_like(part_ref)

        @pl.when((step >= k * steps) & (step < (k + 1) * steps))
        def _():
            grad_block(xt_ref, dy[k], out[3 * k], part_ref, out[3 * k + 2])

        @pl.when(step == (k + 1) * steps - 1)
        def _():
            out[3 * k + 1][...] = jnp.sum(part_ref[...].T, axis=0, keepdims=True)


def weight_grads(x, dys, tile):
    tokens, m = x.shape
    n = dys[0].shape[1]
    steps = n // tile
    count = len(dys)

    def block(k):
        return lambda j: (0, jnp.clip(j - k * steps, 0, steps - 1))

    out_specs, out_shape = [], []
    for k in range(count):
        out_specs += [
            pl.BlockSpec((m, tile), block(k)),
            pl.BlockSpec((1, m), lambda j: (0, 0)),
            pl.BlockSpec((1, tile), block(k)),
        ]
        out_shape += [
            jax.ShapeDtypeStruct((m, n), F32),
            jax.ShapeDtypeStruct((1, m), F32),
            jax.ShapeDtypeStruct((1, n), F32),
        ]
    out = pl.pallas_call(
        functools.partial(grad_kernel, count, steps),
        grid=(steps * count,),
        in_specs=[pl.BlockSpec((tokens, m), lambda j: (0, 0), pipeline_mode=pl.Buffered(1))]
        + [pl.BlockSpec((tokens, tile), block(k)) for k in range(count)],
        out_specs=out_specs,
        out_shape=out_shape,
        scratch_shapes=[pltpu.VMEM((m, tokens), BF16), pltpu.VMEM((m, 128), F32)],
        compiler_params=params('arbitrary'),
        cost_estimate=cost(2 * count * tokens * m * n, count * (2 * tokens * (m + n) + 4 * m * n)),
        name='weight_grads',
    )(x, *dys)
    return [tuple(out[3 * k:3 * k + 3]) for k in range(count)]


def norm_kernel(chunk, start_ref, dyg_ref, dyu_ref, wg_ref, wu_ref, *refs):
    out, squares, (acc_ref, wb_ref, stage_ref, sems) = refs[:4], refs[4:6], refs[6:]
    step = pl.program_id(0)
    weights = (wg_ref, wu_ref)
    chunks = wg_ref.shape[1] // chunk
    slots = stage_ref.shape[0]
    per_out = pl.num_programs(0) // 4

    def fetch(matrix, c):
        slot = lax.rem(matrix * chunks + c, slots)
        cols = pl.ds(pl.multiple_of(c * chunk, chunk), chunk)
        return pltpu.make_async_copy(weights[matrix].at[:, cols], stage_ref.at[slot], sems.at[slot])

    @pl.when(step == 0)
    def _():
        for c in range(slots):
            fetch(0, c).start()
        acc_ref[...] = jnp.zeros_like(acc_ref)
        for k, dy_ref in enumerate((dyg_ref, dyu_ref)):
            squares[k][...] = jnp.zeros_like(squares[k])

            @pl.loop(0, chunks)
            def _(c):
                fetch(k, c).wait()
                slot = lax.rem(k * chunks + c, slots)
                cols = pl.ds(pl.multiple_of(c * chunk, chunk), chunk)
                w = stage_ref[slot]
                wb_ref[k, :, cols] = w.astype(BF16)
                squares[k][...] += fold_squares(w)

                @pl.when(c + slots < chunks)
                def _():
                    fetch(k, c + slots).start()

                if k == 0:
                    @pl.when(c + slots >= chunks)
                    def _():
                        fetch(1, c + slots - chunks).start()

                acc_ref[...] += lax.dot_general(dy_ref[:, cols], wb_ref[k, :, cols], NT, preferred_element_type=F32)

    @pl.when(step > 0)
    def _():
        acc_ref[...] = lax.dot_general(dyg_ref[...], wb_ref[0], NT, preferred_element_type=F32) + lax.dot_general(
            dyu_ref[...], wb_ref[1], NT, preferred_element_type=F32)

    for k in range(4):
        @pl.when((step >= k * per_out) & (step < (k + 1) * per_out))
        def _():
            out[k][...] = acc_ref[...]


def norm_partial(first, dyg, dyu, wg, wu):
    tile, chunk, slots = 512, 1024, 3
    tokens, n = dyg.shape
    m = wg.shape[0]
    tiles = tokens // tile
    per_out = tiles // 4
    dy_spec = pl.BlockSpec((tile, n), lambda i, start: (lax.rem(i + start[0], tiles), 0))
    any_spec = pl.BlockSpec(memory_space=pl.ANY)

    def block(k):
        return lambda i, start: (jnp.clip(i - k * per_out, 0, per_out - 1), 0)

    out = pl.pallas_call(
        functools.partial(norm_kernel, chunk),
        grid_spec=pltpu.PrefetchScalarGridSpec(
            num_scalar_prefetch=1,
            grid=(tiles,),
            in_specs=[dy_spec, dy_spec, any_spec, any_spec],
            out_specs=[pl.BlockSpec((tile, m), block(k)) for k in range(4)]
            + [pl.BlockSpec((8, chunk), lambda i, start: (0, 0))] * 2,
            scratch_shapes=[
                pltpu.VMEM((tile, m), F32),
                pltpu.VMEM((2, m, n), BF16),
                pltpu.VMEM((slots, m, chunk), F32),
                pltpu.SemaphoreType.DMA((slots,)),
            ],
        ),
        out_shape=[jax.ShapeDtypeStruct((tokens // 4, m), F32)] * 4 + [jax.ShapeDtypeStruct((8, chunk), F32)] * 2,
        compiler_params=params('arbitrary'),
        cost_estimate=cost(4 * tokens * m * n, 4 * tokens * n + 8 * m * n + 4 * tokens * m),
        name='norm_partial',
    )((first * (tiles // 2)).astype(jnp.int32).reshape(1), dyg, dyu, wg, wu)
    return out


def lane_fold(v):
    return functools.reduce(lambda p, q: p + q, [v[:, k:k + 128] for k in range(0, v.shape[1], 128)])


def direction(g, r_ref, rows, c_ref):
    r = r_ref[rows, :]
    r = jnp.concatenate([r] * (g.shape[1] // 128), axis=1)
    return g * lax.rsqrt(r * c_ref[...])


def square_kernel(row_total, sizes, hyper_ref, g0, g1, g2, all_ref, r_ref,
                  c0, c1, c2, w0, w1, w2, n0, n1, n2, ratio_ref, part_ref, acc_ref):
    step = pl.program_id(0)
    beta_two = hyper_ref[0]
    grads, c_new = (g0, g1, g2), (n0, n1, n2)
    starts = [0, sizes[0], sizes[0] + sizes[1]]

    @pl.when(step == 0)
    def _():
        off = 0
        for c_old, new, total in zip((c0, c1, c2), c_new, row_total):
            size = c_old.shape[1]
            new[...] = beta_two * c_old[...] + (1.0 - beta_two) * (all_ref[:, off:off + size] / total)
            off += size
        for k in range(3):
            mean = jnp.sum(all_ref[:, off + 128 * k:off + 128 * k + 128], axis=1, keepdims=True) / row_total[k]
            for i in range(starts[k], starts[k] + sizes[k], 128):
                ratio_ref[i:i + 128, :] = jnp.broadcast_to(r_ref[:, i:i + 128] / mean, (128, 128)).T
        acc_ref[...] = jnp.zeros_like(acc_ref)

    for k in range(3):
        tile = grads[k].shape[0]

        @pl.loop(0, tile // 8)
        def _(i):
            g = grads[k][pl.ds(pl.multiple_of(i * 8, 8), 8), :]
            rows = pl.ds(pl.multiple_of(starts[k] + step * tile + i * 8, 8), 8)
            u = direction(g, ratio_ref, rows, c_new[k])
            acc_ref[k] += lane_fold(u * u)

    @pl.when(step == pl.num_programs(0) - 1)
    def _():
        part_ref[...] = jnp.zeros_like(part_ref)
        for k in range(3):
            part_ref[k:k + 1, :] = jnp.sum(acc_ref[k], axis=0, keepdims=True)
        for k, w in enumerate((w0, w1, w2)):
            part_ref[3 + k:4 + k, :] = jnp.sum(lane_fold(w[...]), axis=0, keepdims=True)


def square_sums(hyper_params, grads, all_sums, r_new, c_old, w_sq, row_total):
    steps = 8
    whole = lambda v: pl.BlockSpec(v.shape, lambda i: (0, 0))
    in_specs = (
        [pl.BlockSpec(memory_space=pltpu.SMEM)]
        + [pl.BlockSpec((g.shape[0] // steps, g.shape[1]), lambda i: (i, 0)) for g in grads]
        + [whole(v) for v in (all_sums, r_new, *c_old, *w_sq)]
    )
    out_shape = [jax.ShapeDtypeStruct(c.shape, F32) for c in c_old] + [
        jax.ShapeDtypeStruct((r_new.shape[1], 128), F32),
        jax.ShapeDtypeStruct((8, 128), F32),
    ]
    size = sum(g.size for g in grads)
    out = pl.pallas_call(
        functools.partial(square_kernel, row_total, [g.shape[0] for g in grads]),
        grid=(steps,),
        in_specs=in_specs,
        out_specs=[whole(v) for v in out_shape],
        out_shape=out_shape,
        scratch_shapes=[pltpu.VMEM((3, 8, 128), F32)],
        compiler_params=params('arbitrary'),
        cost_estimate=cost(1000 * size, 4 * size),
        name='square_sums',
    )(hyper_params, *grads, all_sums, r_new, *c_old, *w_sq)
    return out[:3], out[3], out[4]


def act_kernel(parts, total, hyper_ref, dya_ref, dyb_ref, *refs):
    w_refs, refs = refs[:2 * parts], refs[2 * parts:]
    weights, grads, c_new, (ratio_ref, sum_ref) = refs[:3], refs[3:6], refs[6:9], refs[9:11]
    out_ref, new, (acc_ref, scale_ref) = refs[11], refs[12:15], refs[15:]
    step = pl.program_id(0)

    @pl.when(step == 0)
    def _():
        mean = jnp.sum(sum_ref[...], axis=1, keepdims=True) / total
        for k in range(3):
            rms_u, rms_w = jnp.sqrt(mean[k:k + 1]), jnp.sqrt(mean[3 + k:4 + k])
            scale = hyper_ref[1] * jnp.maximum(EPS_TWO, rms_w) / jnp.maximum(1.0, rms_u / hyper_ref[2])
            scale_ref[k] = jnp.broadcast_to(scale, (8, 128))

    def halves(dy_ref, refs):
        done = 0
        for w_ref in refs:
            yield slice(done, done + w_ref.shape[0]), lax.dot_general(
                dy_ref[...], w_ref[...], NT, preferred_element_type=F32)
            done += w_ref.shape[0]

    @pl.when(step >= 0)
    def _():
        for cols, part in halves(dya_ref, w_refs[:parts]):
            acc_ref[:, cols] = part

    @pl.when(step < pl.num_programs(0))
    def _():
        for cols, part in halves(dyb_ref, w_refs[parts:]):
            out_ref[:, cols] = (acc_ref[:, cols] + part).astype(BF16)

    start = 0
    for k in range(3):
        tile, n = weights[k].shape

        @pl.loop(0, tile // 8)
        def _(i):
            slab = pl.ds(pl.multiple_of(i * 8, 8), 8)
            rows = pl.ds(pl.multiple_of(start + step * tile + i * 8, 8), 8)
            u = direction(grads[k][slab, :], ratio_ref, rows, c_new[k])
            scale = jnp.concatenate([scale_ref[k]] * (n // 128), axis=1)
            new[k][slab, :] = weights[k][slab, :] - scale * u

        start += tile * pl.num_programs(0)


def act_and_update(hyper_params, dya, dyb, wa, wb, weights, grads, c_new, ratio, sums, total):
    tile = 512
    tokens, n = dya.shape
    steps = tokens // tile
    m = sum(w.shape[0] for w in wa)
    dy_spec = pl.BlockSpec((tile, n), lambda i: (i, 0))
    fixed = lambda v: pl.BlockSpec(v.shape, lambda i: (0, 0), pipeline_mode=pl.Buffered(1))
    rows = lambda v: pl.BlockSpec((v.shape[0] // steps, v.shape[1]), lambda i: (i, 0))
    size = sum(w.size for w in weights)
    out = pl.pallas_call(
        functools.partial(act_kernel, len(wa), total),
        grid=(steps,),
        in_specs=[pl.BlockSpec(memory_space=pltpu.SMEM), dy_spec, dy_spec]
        + [fixed(w) for w in (*wa, *wb)]
        + [rows(v) for v in (*weights, *grads)]
        + [fixed(v) for v in (*c_new, ratio, sums)],
        out_specs=[pl.BlockSpec((tile, m), lambda i: (i, 0))] + [rows(w) for w in weights],
        out_shape=[jax.ShapeDtypeStruct((tokens, m), BF16)] + [jax.ShapeDtypeStruct(w.shape, F32) for w in weights],
        scratch_shapes=[pltpu.VMEM((tile, m), F32), pltpu.VMEM((3, 8, 128), F32)],
        compiler_params=params('arbitrary'),
        cost_estimate=cost(4 * tokens * m * n, 4 * tokens * n + 4 * m * n + 2 * tokens * m + 12 * size),
        name='act_and_update',
    )(hyper_params, dya, dyb, *wa, *wb, *weights, *grads, *c_new, ratio, sums)
    return out[0], out[1:]


def swap_col(v):
    return lax.ppermute(v, 'col', [(0, 1), (1, 0)])


def sum_row(v, row_size):
    step = 1
    while step < row_size:
        v = v + lax.ppermute(v, 'row', [(i, i ^ step) for i in range(row_size)])
        step *= 2
    return v


def solution(mesh):
    row_size = mesh.shape['row']
    col_size = mesh.shape['col']
    weight_spec = P('row', 'col')
    act_spec = P(None, 'row')
    grad_spec = P(None, 'col')
    in_specs = (weight_spec,) * 3 + (act_spec, act_spec) + (grad_spec,) * 3 + (P('row'), P('col')) * 3 + (P(),)
    out_specs = (weight_spec,) * 3 + (P('row'), P('col')) * 3 + (act_spec, act_spec)

    def body(w_gate, w_up, w_down, x_norm, x_act, dy_gate, dy_up, dy_down, r_gate, c_gate, r_up, c_up, r_down, c_down, hyper_params):
        row = lax.axis_index('row')
        col = lax.axis_index('col')
        tokens = x_norm.shape[0]
        half = tokens // col_size
        beta_two = hyper_params[0]

        share = tokens // row_size
        piece = lax.dynamic_slice_in_dim(dy_down, row * share, share, axis=0)
        piece = swap_col(piece)
        dy_down_other = lax.all_gather(piece, 'row', axis=0, tiled=True)
        b_down_a, b_down_b, w_sq_down = cast_weight(w_down, 768)
        o_down_a = swap_col(b_down_a)

        (g_gate, row_gate, col_gate), (g_up, row_up, col_up) = weight_grads(x_norm, [dy_gate, dy_up], 512)
        ((g_down, row_down, col_down),) = weight_grads(x_act, [dy_down], 256)
        row_all = jnp.concatenate([row_gate, row_up, row_down], axis=1)
        row_peer = swap_col(row_all)
        o_down_b = swap_col(b_down_b)
        sent0, sent1, own0, own1, w_sq_gate, w_sq_up = norm_partial(1 - col, dy_gate, dy_up, w_gate, w_up)
        got0 = swap_col(sent0)

        got1 = swap_col(sent1)

        sizes = [r_gate.shape[0], r_up.shape[0], r_down.shape[0]]
        bounds = [0, sizes[0], sizes[0] + sizes[1], sum(sizes)]
        row_total = [v * row_size for v in sizes]
        col_total = [v.shape[0] * col_size for v in (c_gate, c_up, c_down)]
        index = lax.broadcasted_iota(jnp.int32, row_all.shape, 1)
        length = jnp.where(index < bounds[1], col_total[0], jnp.where(index < bounds[2], col_total[1], col_total[2]))
        r_old = jnp.concatenate([r_gate, r_up, r_down])[None]
        r_new = beta_two * r_old + (1.0 - beta_two) * ((row_all + row_peer) / length.astype(F32))
        r_part = [lane_fold(r_new[:, bounds[k]:bounds[k + 1]]) for k in range(3)]
        all_sums = sum_row(jnp.concatenate([col_gate, col_up, col_down, *r_part], axis=1), row_size)
        grads = [g_gate, g_up, g_down]
        c_new, ratio, sums = square_sums(
            hyper_params, grads, all_sums, r_new, [c_gate[None], c_up[None], c_down[None]],
            [w_sq_gate, w_sq_up, w_sq_down], row_total)
        sums = sum_row(sums, row_size)
        sums_peer = swap_col(sums)
        dx_act, new = act_and_update(
            hyper_params, dy_down, dy_down_other, [b_down_a, b_down_b], [o_down_a, o_down_b],
            [w_gate, w_up, w_down], grads, c_new, ratio, sums + sums_peer, float(row_total[0] * col_total[0]))
        r_new = [r_new[0, bounds[k]:bounds[k + 1]] for k in range(3)]
        c_new = [c[0] for c in c_new]

        mine0 = (own0 + got0).astype(BF16)
        theirs0 = swap_col(mine0)
        mine1 = (own1 + got1).astype(BF16)
        theirs1 = swap_col(mine1)
        dx_norm = jnp.where(
            col == 0,
            jnp.concatenate([mine0, mine1, theirs0, theirs0]),
            jnp.concatenate([theirs0, theirs0, mine0, mine1]),
        )
        dx_norm = lax.dynamic_update_slice_in_dim(dx_norm, theirs1, (1 - col) * half + half // 2, axis=0)
        return (*new, r_new[0], c_new[0], r_new[1], c_new[1], r_new[2], c_new[2], dx_norm, dx_act)

    return jax.shard_map(body, mesh=mesh, in_specs=in_specs, out_specs=out_specs, check_vma=False)
```

```python
import functools

import jax
import jax.numpy as jnp
from jax import lax
from jax.experimental import pallas as pl
from jax.experimental.pallas import tpu as pltpu
from jax.sharding import PartitionSpec as P

EPS_ONE = 1e-30
EPS_TWO = 1e-3
F32 = jnp.float32
BF16 = jnp.bfloat16
VMEM_LIMIT = 60 * 1024 * 1024
NT = (((1,), (1,)), ((), ()))


def params(*semantics):
    return pltpu.CompilerParams(dimension_semantics=semantics, vmem_limit_bytes=VMEM_LIMIT)


def cost(flops, nbytes):
    return pl.CostEstimate(flops=int(flops), bytes_accessed=int(nbytes), transcendentals=0)


def fold_squares(v):
    return jnp.sum((v * v).reshape(v.shape[0] // 8, 8, v.shape[1]), axis=0)


def cast_kernel(first, w_ref, a_ref, b_ref, s_ref):
    step = pl.program_id(0)
    w = w_ref[...]

    @pl.when(step < first)
    def _():
        a_ref[...] = w.astype(BF16)

    @pl.when(step >= first)
    def _():
        b_ref[...] = w.astype(BF16)

    @pl.when(step == 0)
    def _():
        s_ref[...] = jnp.zeros_like(s_ref)

    s_ref[...] += fold_squares(w)


def cast_weight(w, cut):
    rows, cols = w.shape
    tile = 256
    first = cut // tile
    a, b, s = pl.pallas_call(
        functools.partial(cast_kernel, first),
        grid=(rows // tile,),
        in_specs=[pl.BlockSpec((tile, cols), lambda i: (i, 0))],
        out_specs=[
            pl.BlockSpec((tile, cols), lambda i: (jnp.minimum(i, first - 1), 0)),
            pl.BlockSpec((tile, cols), lambda i: (jnp.maximum(i - first, 0), 0)),
            pl.BlockSpec((8, cols), lambda i: (0, 0)),
        ],
        out_shape=[
            jax.ShapeDtypeStruct((cut, cols), BF16),
            jax.ShapeDtypeStruct((rows - cut, cols), BF16),
            jax.ShapeDtypeStruct((8, cols), F32),
        ],
        compiler_params=params('arbitrary'),
        cost_estimate=cost(w.size * 1000, w.size * 6),
        name='cast_weight',
    )(w)
    return a, b, s


def grad_block(xt_ref, dy_ref, g_ref, row_ref, col_ref):
    g = jnp.dot(xt_ref[...], dy_ref[...], preferred_element_type=F32)
    g_ref[...] = g
    q = g * g + EPS_ONE
    col_ref[...] = jnp.sum(q, axis=0, keepdims=True)
    part = q[:, :128]
    for k in range(1, q.shape[1] // 128):
        part += q[:, k * 128:(k + 1) * 128]
    row_ref[...] += part


def grad_kernel(count, steps, x_ref, *refs):
    dy, out, xt_ref, part_ref = refs[:count], refs[count:-2], refs[-2], refs[-1]
    step = pl.program_id(0)

    @pl.when(step == 0)
    def _():
        xt_ref[...] = x_ref[...].T

    for k in range(count):
        @pl.when(step == k * steps)
        def _():
            part_ref[...] = jnp.zeros_like(part_ref)

        @pl.when((step >= k * steps) & (step < (k + 1) * steps))
        def _():
            grad_block(xt_ref, dy[k], out[3 * k], part_ref, out[3 * k + 2])

        @pl.when(step == (k + 1) * steps - 1)
        def _():
            out[3 * k + 1][...] = jnp.sum(part_ref[...].T, axis=0, keepdims=True)


def weight_grads(x, dys, tile):
    tokens, m = x.shape
    n = dys[0].shape[1]
    steps = n // tile
    count = len(dys)

    def block(k):
        return lambda j: (0, jnp.clip(j - k * steps, 0, steps - 1))

    out_specs, out_shape = [], []
    for k in range(count):
        out_specs += [
            pl.BlockSpec((m, tile), block(k)),
            pl.BlockSpec((1, m), lambda j: (0, 0)),
            pl.BlockSpec((1, tile), block(k)),
        ]
        out_shape += [
            jax.ShapeDtypeStruct((m, n), F32),
            jax.ShapeDtypeStruct((1, m), F32),
            jax.ShapeDtypeStruct((1, n), F32),
        ]
    out = pl.pallas_call(
        functools.partial(grad_kernel, count, steps),
        grid=(steps * count,),
        in_specs=[pl.BlockSpec((tokens, m), lambda j: (0, 0), pipeline_mode=pl.Buffered(1))]
        + [pl.BlockSpec((tokens, tile), block(k)) for k in range(count)],
        out_specs=out_specs,
        out_shape=out_shape,
        scratch_shapes=[pltpu.VMEM((m, tokens), BF16), pltpu.VMEM((m, 128), F32)],
        compiler_params=params('arbitrary'),
        cost_estimate=cost(2 * count * tokens * m * n, count * (2 * tokens * (m + n) + 4 * m * n)),
        name='weight_grads',
    )(x, *dys)
    return [tuple(out[3 * k:3 * k + 3]) for k in range(count)]


def norm_kernel(chunk, start_ref, dyg_ref, dyu_ref, wg_ref, wu_ref, *refs):
    out, squares, (acc_ref, wb_ref, stage_ref, sems) = refs[:4], refs[4:6], refs[6:]
    step = pl.program_id(0)
    weights = (wg_ref, wu_ref)
    chunks = wg_ref.shape[1] // chunk
    slots = stage_ref.shape[0]
    per_out = pl.num_programs(0) // 4

    def fetch(matrix, c):
        slot = lax.rem(matrix * chunks + c, slots)
        cols = pl.ds(pl.multiple_of(c * chunk, chunk), chunk)
        return pltpu.make_async_copy(weights[matrix].at[:, cols], stage_ref.at[slot], sems.at[slot])

    @pl.when(step == 0)
    def _():
        for c in range(slots):
            fetch(0, c).start()
        acc_ref[...] = jnp.zeros_like(acc_ref)
        for k, dy_ref in enumerate((dyg_ref, dyu_ref)):
            squares[k][...] = jnp.zeros_like(squares[k])

            @pl.loop(0, chunks)
            def _(c):
                fetch(k, c).wait()
                slot = lax.rem(k * chunks + c, slots)
                cols = pl.ds(pl.multiple_of(c * chunk, chunk), chunk)
                w = stage_ref[slot]
                wb_ref[k, :, cols] = w.astype(BF16)
                squares[k][...] += fold_squares(w)

                @pl.when(c + slots < chunks)
                def _():
                    fetch(k, c + slots).start()

                if k == 0:
                    @pl.when(c + slots >= chunks)
                    def _():
                        fetch(1, c + slots - chunks).start()

                acc_ref[...] += lax.dot_general(dy_ref[:, cols], wb_ref[k, :, cols], NT, preferred_element_type=F32)

    @pl.when(step > 0)
    def _():
        acc_ref[...] = lax.dot_general(dyg_ref[...], wb_ref[0], NT, preferred_element_type=F32) + lax.dot_general(
            dyu_ref[...], wb_ref[1], NT, preferred_element_type=F32)

    for k in range(4):
        @pl.when((step >= k * per_out) & (step < (k + 1) * per_out))
        def _():
            out[k][...] = acc_ref[...]


def norm_partial(first, dyg, dyu, wg, wu):
    tile, chunk, slots = 512, 1024, 3
    tokens, n = dyg.shape
    m = wg.shape[0]
    tiles = tokens // tile
    per_out = tiles // 4
    dy_spec = pl.BlockSpec((tile, n), lambda i, start: (lax.rem(i + start[0], tiles), 0))
    any_spec = pl.BlockSpec(memory_space=pl.ANY)

    def block(k):
        return lambda i, start: (jnp.clip(i - k * per_out, 0, per_out - 1), 0)

    out = pl.pallas_call(
        functools.partial(norm_kernel, chunk),
        grid_spec=pltpu.PrefetchScalarGridSpec(
            num_scalar_prefetch=1,
            grid=(tiles,),
            in_specs=[dy_spec, dy_spec, any_spec, any_spec],
            out_specs=[pl.BlockSpec((tile, m), block(k)) for k in range(4)]
            + [pl.BlockSpec((8, chunk), lambda i, start: (0, 0))] * 2,
            scratch_shapes=[
                pltpu.VMEM((tile, m), F32),
                pltpu.VMEM((2, m, n), BF16),
                pltpu.VMEM((slots, m, chunk), F32),
                pltpu.SemaphoreType.DMA((slots,)),
            ],
        ),
        out_shape=[jax.ShapeDtypeStruct((tokens // 4, m), F32)] * 4 + [jax.ShapeDtypeStruct((8, chunk), F32)] * 2,
        compiler_params=params('arbitrary'),
        cost_estimate=cost(4 * tokens * m * n, 4 * tokens * n + 8 * m * n + 4 * tokens * m),
        name='norm_partial',
    )((first * (tiles // 2)).astype(jnp.int32).reshape(1), dyg, dyu, wg, wu)
    return out


def lane_fold(v):
    parts = [v[:, k:k + 128] for k in range(0, v.shape[1], 128)]
    while len(parts) > 1:
        parts = [p + q for p, q in zip(parts[::2], parts[1::2])] + parts[len(parts) & ~1:]
    return parts[0]


def direction(g, r_ref, rows, c_ref):
    r = r_ref[rows, :]
    r = jnp.concatenate([r] * (g.shape[1] // 128), axis=1)
    return g * lax.rsqrt(r * c_ref[...])


def square_kernel(row_total, sizes, hyper_ref, g0, g1, g2, all_ref, r_ref,
                  c0, c1, c2, w0, w1, w2, n0, n1, n2, ratio_ref, part_ref, acc_ref):
    step = pl.program_id(0)
    beta_two = hyper_ref[0]
    grads, c_new = (g0, g1, g2), (n0, n1, n2)
    starts = [0, sizes[0], sizes[0] + sizes[1]]

    @pl.when(step == 0)
    def _():
        off = 0
        for c_old, new, total in zip((c0, c1, c2), c_new, row_total):
            size = c_old.shape[1]
            new[...] = beta_two * c_old[...] + (1.0 - beta_two) * (all_ref[:, off:off + size] / total)
            off += size
        for k in range(3):
            mean = jnp.sum(all_ref[:, off + 128 * k:off + 128 * k + 128], axis=1, keepdims=True) / row_total[k]
            for i in range(starts[k], starts[k] + sizes[k], 128):
                ratio_ref[i:i + 128, :] = jnp.broadcast_to(r_ref[:, i:i + 128] / mean, (128, 128)).T
        acc_ref[...] = jnp.zeros_like(acc_ref)

    for k in range(3):
        tile = grads[k].shape[0]

        @pl.loop(0, tile // 8, unroll=4)
        def _(i):
            g = grads[k][pl.ds(pl.multiple_of(i * 8, 8), 8), :]
            rows = pl.ds(pl.multiple_of(starts[k] + step * tile + i * 8, 8), 8)
            u = direction(g, ratio_ref, rows, c_new[k])
            acc_ref[k] += lane_fold(u * u)

    @pl.when(step == pl.num_programs(0) - 1)
    def _():
        part_ref[...] = jnp.zeros_like(part_ref)
        for k in range(3):
            part_ref[k:k + 1, :] = jnp.sum(acc_ref[k], axis=0, keepdims=True)
        for k, w in enumerate((w0, w1, w2)):
            part_ref[3 + k:4 + k, :] = jnp.sum(lane_fold(w[...]), axis=0, keepdims=True)


def square_sums(hyper_params, grads, all_sums, r_new, c_old, w_sq, row_total):
    steps = 8
    whole = lambda v: pl.BlockSpec(v.shape, lambda i: (0, 0))
    in_specs = (
        [pl.BlockSpec(memory_space=pltpu.SMEM)]
        + [pl.BlockSpec((g.shape[0] // steps, g.shape[1]), lambda i: (i, 0)) for g in grads]
        + [whole(v) for v in (all_sums, r_new, *c_old, *w_sq)]
    )
    out_shape = [jax.ShapeDtypeStruct(c.shape, F32) for c in c_old] + [
        jax.ShapeDtypeStruct((r_new.shape[1], 128), F32),
        jax.ShapeDtypeStruct((8, 128), F32),
    ]
    size = sum(g.size for g in grads)
    out = pl.pallas_call(
        functools.partial(square_kernel, row_total, [g.shape[0] for g in grads]),
        grid=(steps,),
        in_specs=in_specs,
        out_specs=[whole(v) for v in out_shape],
        out_shape=out_shape,
        scratch_shapes=[pltpu.VMEM((3, 8, 128), F32)],
        compiler_params=params('arbitrary'),
        cost_estimate=cost(1000 * size, 4 * size),
        name='square_sums',
    )(hyper_params, *grads, all_sums, r_new, *c_old, *w_sq)
    return out[:3], out[3], out[4]


def act_kernel(parts, total, hyper_ref, dya_ref, dyb_ref, *refs):
    w_refs, refs = refs[:2 * parts], refs[2 * parts:]
    weights, grads, c_new, (ratio_ref, sum_ref) = refs[:3], refs[3:6], refs[6:9], refs[9:11]
    out_ref, new, (acc_ref, scale_ref) = refs[11], refs[12:15], refs[15:]
    step = pl.program_id(0)

    @pl.when(step == 0)
    def _():
        mean = jnp.sum(sum_ref[...], axis=1, keepdims=True) / total
        for k in range(3):
            rms_u, rms_w = jnp.sqrt(mean[k:k + 1]), jnp.sqrt(mean[3 + k:4 + k])
            scale = hyper_ref[1] * jnp.maximum(EPS_TWO, rms_w) / jnp.maximum(1.0, rms_u / hyper_ref[2])
            scale_ref[k] = jnp.broadcast_to(scale, (8, 128))

    def halves(dy_ref, refs):
        done = 0
        for w_ref in refs:
            yield slice(done, done + w_ref.shape[0]), lax.dot_general(
                dy_ref[...], w_ref[...], NT, preferred_element_type=F32)
            done += w_ref.shape[0]

    @pl.when(step >= 0)
    def _():
        for cols, part in halves(dya_ref, w_refs[:parts]):
            acc_ref[:, cols] = part

    @pl.when(step < pl.num_programs(0))
    def _():
        for cols, part in halves(dyb_ref, w_refs[parts:]):
            out_ref[:, cols] = (acc_ref[:, cols] + part).astype(BF16)

    start = 0
    for k in range(3):
        tile, n = weights[k].shape

        @pl.loop(0, tile // 8, unroll=4)
        def _(i):
            slab = pl.ds(pl.multiple_of(i * 8, 8), 8)
            rows = pl.ds(pl.multiple_of(start + step * tile + i * 8, 8), 8)
            u = direction(grads[k][slab, :], ratio_ref, rows, c_new[k])
            scale = jnp.concatenate([scale_ref[k]] * (n // 128), axis=1)
            new[k][slab, :] = weights[k][slab, :] - scale * u

        start += tile * pl.num_programs(0)


def act_and_update(hyper_params, dya, dyb, wa, wb, weights, grads, c_new, ratio, sums, total):
    tile = 512
    tokens, n = dya.shape
    steps = tokens // tile
    m = sum(w.shape[0] for w in wa)
    dy_spec = pl.BlockSpec((tile, n), lambda i: (i, 0))
    fixed = lambda v: pl.BlockSpec(v.shape, lambda i: (0, 0), pipeline_mode=pl.Buffered(1))
    rows = lambda v: pl.BlockSpec((v.shape[0] // steps, v.shape[1]), lambda i: (i, 0))
    size = sum(w.size for w in weights)
    out = pl.pallas_call(
        functools.partial(act_kernel, len(wa), total),
        grid=(steps,),
        in_specs=[pl.BlockSpec(memory_space=pltpu.SMEM), dy_spec, dy_spec]
        + [fixed(w) for w in (*wa, *wb)]
        + [rows(v) for v in (*weights, *grads)]
        + [fixed(v) for v in (*c_new, ratio, sums)],
        out_specs=[pl.BlockSpec((tile, m), lambda i: (i, 0))] + [rows(w) for w in weights],
        out_shape=[jax.ShapeDtypeStruct((tokens, m), BF16)] + [jax.ShapeDtypeStruct(w.shape, F32) for w in weights],
        scratch_shapes=[pltpu.VMEM((tile, m), F32), pltpu.VMEM((3, 8, 128), F32)],
        compiler_params=params('arbitrary'),
        cost_estimate=cost(4 * tokens * m * n, 4 * tokens * n + 4 * m * n + 2 * tokens * m + 12 * size),
        name='act_and_update',
    )(hyper_params, dya, dyb, *wa, *wb, *weights, *grads, *c_new, ratio, sums)
    return out[0], out[1:]


def swap_col(v):
    return lax.ppermute(v, 'col', [(0, 1), (1, 0)])


def sum_row(v, row_size):
    step = 1
    while step < row_size:
        v = v + lax.ppermute(v, 'row', [(i, i ^ step) for i in range(row_size)])
        step *= 2
    return v


def solution(mesh):
    row_size = mesh.shape['row']
    col_size = mesh.shape['col']
    weight_spec = P('row', 'col')
    act_spec = P(None, 'row')
    grad_spec = P(None, 'col')
    in_specs = (weight_spec,) * 3 + (act_spec, act_spec) + (grad_spec,) * 3 + (P('row'), P('col')) * 3 + (P(),)
    out_specs = (weight_spec,) * 3 + (P('row'), P('col')) * 3 + (act_spec, act_spec)

    def body(w_gate, w_up, w_down, x_norm, x_act, dy_gate, dy_up, dy_down, r_gate, c_gate, r_up, c_up, r_down, c_down, hyper_params):
        row = lax.axis_index('row')
        col = lax.axis_index('col')
        tokens = x_norm.shape[0]
        half = tokens // col_size
        beta_two = hyper_params[0]

        share = tokens // row_size
        piece = lax.dynamic_slice_in_dim(dy_down, row * share, share, axis=0)
        piece = swap_col(piece)
        dy_down_other = lax.all_gather(piece, 'row', axis=0, tiled=True)
        b_down_a, b_down_b, w_sq_down = cast_weight(w_down, 768)
        o_down_a = swap_col(b_down_a)

        (g_gate, row_gate, col_gate), (g_up, row_up, col_up) = weight_grads(x_norm, [dy_gate, dy_up], 512)
        ((g_down, row_down, col_down),) = weight_grads(x_act, [dy_down], 512)
        row_all = jnp.concatenate([row_gate, row_up, row_down], axis=1)
        row_peer = swap_col(row_all)
        o_down_b = swap_col(b_down_b)
        sent0, sent1, own0, own1, w_sq_gate, w_sq_up = norm_partial(1 - col, dy_gate, dy_up, w_gate, w_up)
        got0 = swap_col(sent0)

        got1 = swap_col(sent1)

        sizes = [r_gate.shape[0], r_up.shape[0], r_down.shape[0]]
        bounds = [0, sizes[0], sizes[0] + sizes[1], sum(sizes)]
        row_total = [v * row_size for v in sizes]
        col_total = [v.shape[0] * col_size for v in (c_gate, c_up, c_down)]
        index = lax.broadcasted_iota(jnp.int32, row_all.shape, 1)
        length = jnp.where(index < bounds[1], col_total[0], jnp.where(index < bounds[2], col_total[1], col_total[2]))
        r_old = jnp.concatenate([r_gate, r_up, r_down])[None]
        r_new = beta_two * r_old + (1.0 - beta_two) * ((row_all + row_peer) / length.astype(F32))
        r_part = [lane_fold(r_new[:, bounds[k]:bounds[k + 1]]) for k in range(3)]
        all_sums = sum_row(jnp.concatenate([col_gate, col_up, col_down, *r_part], axis=1), row_size)
        grads = [g_gate, g_up, g_down]
        c_new, ratio, sums = square_sums(
            hyper_params, grads, all_sums, r_new, [c_gate[None], c_up[None], c_down[None]],
            [w_sq_gate, w_sq_up, w_sq_down], row_total)
        sums = sum_row(sums, row_size)
        sums_peer = swap_col(sums)
        dx_act, new = act_and_update(
            hyper_params, dy_down, dy_down_other, [b_down_a, b_down_b], [o_down_a, o_down_b],
            [w_gate, w_up, w_down], grads, c_new, ratio, sums + sums_peer, float(row_total[0] * col_total[0]))
        r_new = [r_new[0, bounds[k]:bounds[k + 1]] for k in range(3)]
        c_new = [c[0] for c in c_new]

        mine0 = (own0 + got0).astype(BF16)
        theirs0 = swap_col(mine0)
        mine1 = (own1 + got1).astype(BF16)
        theirs1 = swap_col(mine1)
        dx_norm = jnp.where(
            col == 0,
            jnp.concatenate([mine0, mine1, theirs0, theirs0]),
            jnp.concatenate([theirs0, theirs0, mine0, mine1]),
        )
        dx_norm = lax.dynamic_update_slice_in_dim(dx_norm, theirs1, (1 - col) * half + half // 2, axis=0)
        return (*new, r_new[0], c_new[0], r_new[1], c_new[1], r_new[2], c_new[2], dx_norm, dx_act)

    return jax.shard_map(body, mesh=mesh, in_specs=in_specs, out_specs=out_specs, check_vma=False)
```

```python
import functools

import jax
import jax.numpy as jnp
from jax import lax
from jax.experimental import pallas as pl
from jax.experimental.pallas import tpu as pltpu
from jax.sharding import PartitionSpec as P


EPS_ONE = 1e-30
EPS_TWO = 1e-3
F32 = jnp.float32
BF16 = jnp.bfloat16
VMEM_LIMIT = 60 * 1024 * 1024
NT = (((1,), (1,)), ((), ()))


def params(*semantics):
    return pltpu.CompilerParams(dimension_semantics=semantics, vmem_limit_bytes=VMEM_LIMIT)


def cost(flops, nbytes):
    return pl.CostEstimate(flops=int(flops), bytes_accessed=int(nbytes), transcendentals=0)


def fold_squares(v):
    return jnp.sum((v * v).reshape(v.shape[0] // 8, 8, v.shape[1]), axis=0)


def cast_kernel(w_ref, b_ref, s_ref):
    w = w_ref[...]
    b_ref[...] = w.astype(BF16)

    @pl.when(pl.program_id(0) == 0)
    def _():
        s_ref[...] = jnp.zeros_like(s_ref)

    s_ref[...] += fold_squares(w)


def cast_weight(w):
    rows, cols = w.shape
    tile = 256
    return pl.pallas_call(
        cast_kernel,
        grid=(rows // tile,),
        in_specs=[pl.BlockSpec((tile, cols), lambda i: (i, 0))],
        out_specs=[pl.BlockSpec((tile, cols), lambda i: (i, 0)), pl.BlockSpec((8, cols), lambda i: (0, 0))],
        out_shape=[jax.ShapeDtypeStruct((rows, cols), BF16), jax.ShapeDtypeStruct((8, cols), F32)],
        compiler_params=params('arbitrary'),
        cost_estimate=cost(w.size * 1000, w.size * 6),
        name='cast_weight',
    )(w)


def grad_block(xt_ref, dy_ref, g_ref, row_ref, col_ref):
    g = jnp.dot(xt_ref[...], dy_ref[...], preferred_element_type=F32)
    g_ref[...] = g
    q = g * g + EPS_ONE
    col_ref[...] = jnp.sum(q, axis=0, keepdims=True)
    part = q[:, :128]
    for k in range(1, q.shape[1] // 128):
        part += q[:, k * 128:(k + 1) * 128]
    row_ref[...] += part


def grad_kernel(count, steps, x_ref, *refs):
    dy, out, xt_ref, part_ref = refs[:count], refs[count:-2], refs[-2], refs[-1]
    step = pl.program_id(0)

    @pl.when(step == 0)
    def _():
        xt_ref[...] = x_ref[...].T

    for k in range(count):
        @pl.when(step == k * steps)
        def _():
            part_ref[...] = jnp.zeros_like(part_ref)

        @pl.when((step >= k * steps) & (step < (k + 1) * steps))
        def _():
            grad_block(xt_ref, dy[k], out[3 * k], part_ref, out[3 * k + 2])

        @pl.when(step == (k + 1) * steps - 1)
        def _():
            out[3 * k + 1][...] = jnp.sum(part_ref[...].T, axis=0, keepdims=True)


def weight_grads(x, dys, tile):
    tokens, m = x.shape
    n = dys[0].shape[1]
    steps = n // tile
    count = len(dys)

    def block(k):
        return lambda j: (0, jnp.clip(j - k * steps, 0, steps - 1))

    out_specs, out_shape = [], []
    for k in range(count):
        out_specs += [
            pl.BlockSpec((m, tile), block(k)),
            pl.BlockSpec((1, m), lambda j: (0, 0)),
            pl.BlockSpec((1, tile), block(k)),
        ]
        out_shape += [
            jax.ShapeDtypeStruct((m, n), F32),
            jax.ShapeDtypeStruct((1, m), F32),
            jax.ShapeDtypeStruct((1, n), F32),
        ]
    out = pl.pallas_call(
        functools.partial(grad_kernel, count, steps),
        grid=(steps * count,),
        in_specs=[pl.BlockSpec((tokens, m), lambda j: (0, 0), pipeline_mode=pl.Buffered(1))]
        + [pl.BlockSpec((tokens, tile), block(k)) for k in range(count)],
        out_specs=out_specs,
        out_shape=out_shape,
        scratch_shapes=[pltpu.VMEM((m, tokens), BF16), pltpu.VMEM((m, 128), F32)],
        compiler_params=params('arbitrary'),
        cost_estimate=cost(2 * count * tokens * m * n, count * (2 * tokens * (m + n) + 4 * m * n)),
        name='weight_grads',
    )(x, *dys)
    return [tuple(out[3 * k:3 * k + 3]) for k in range(count)]


def norm_kernel(chunk, start_ref, dyg_ref, dyu_ref, wg_ref, wu_ref, *refs):
    out, squares, (acc_ref, wb_ref, stage_ref, sems) = refs[:-6], refs[-6:-4], refs[-4:]
    step = pl.program_id(0)
    weights = (wg_ref, wu_ref)
    chunks = wg_ref.shape[1] // chunk
    slots = stage_ref.shape[0]
    tile = dyg_ref.shape[0]

    def fetch(matrix, c):
        slot = lax.rem(matrix * chunks + c, slots)
        cols = pl.ds(pl.multiple_of(c * chunk, chunk), chunk)
        return pltpu.make_async_copy(weights[matrix].at[:, cols], stage_ref.at[slot], sems.at[slot])

    @pl.when(step == 0)
    def _():
        for c in range(slots):
            fetch(0, c).start()
        acc_ref[...] = jnp.zeros_like(acc_ref)
        for k, dy_ref in enumerate((dyg_ref, dyu_ref)):
            squares[k][...] = jnp.zeros_like(squares[k])

            @pl.loop(0, chunks)
            def _(c):
                fetch(k, c).wait()
                slot = lax.rem(k * chunks + c, slots)
                cols = pl.ds(pl.multiple_of(c * chunk, chunk), chunk)
                w = stage_ref[slot]
                wb_ref[k, :, cols] = w.astype(BF16)
                squares[k][...] += fold_squares(w)

                @pl.when(c + slots < chunks)
                def _():
                    fetch(k, c + slots).start()

                if k == 0:
                    @pl.when(c + slots >= chunks)
                    def _():
                        fetch(1, c + slots - chunks).start()

                acc_ref[...] += lax.dot_general(dy_ref[:, cols], wb_ref[k, :, cols], NT, preferred_element_type=F32)

    @pl.when(step > 0)
    def _():
        acc_ref[...] = lax.dot_general(dyg_ref[...], wb_ref[0], NT, preferred_element_type=F32) + lax.dot_general(
            dyu_ref[...], wb_ref[1], NT, preferred_element_type=F32)

    at = 0
    for ref in out:
        for lo in range(at - at % tile, at + ref.shape[0], tile):
            first, last = max(lo, at), min(lo + tile, at + ref.shape[0])

            @pl.when(step == lo // tile)
            def _():
                ref[first - at:last - at, :] = acc_ref[first - lo:last - lo, :]

        at += ref.shape[0]


def norm_partial(first, dyg, dyu, wg, wu, counts):
    tile, chunk, slots = 512, 1024, 3
    tokens, n = dyg.shape
    m = wg.shape[0]
    tiles = tokens // tile
    dy_spec = pl.BlockSpec((tile, n), lambda i, start: (lax.rem(i + start[0], tiles), 0))
    any_spec = pl.BlockSpec(memory_space=pl.ANY)

    out = pl.pallas_call(
        functools.partial(norm_kernel, chunk),
        grid_spec=pltpu.PrefetchScalarGridSpec(
            num_scalar_prefetch=1,
            grid=(tiles,),
            in_specs=[dy_spec, dy_spec, any_spec, any_spec],
            out_specs=[pl.BlockSpec((c, m), lambda i, start: (0, 0)) for c in counts]
            + [pl.BlockSpec((8, chunk), lambda i, start: (0, 0))] * 2,
            scratch_shapes=[
                pltpu.VMEM((tile, m), F32),
                pltpu.VMEM((2, m, n), BF16),
                pltpu.VMEM((slots, m, chunk), F32),
                pltpu.SemaphoreType.DMA((slots,)),
            ],
        ),
        out_shape=[jax.ShapeDtypeStruct((c, m), F32) for c in counts] + [jax.ShapeDtypeStruct((8, chunk), F32)] * 2,
        compiler_params=params('arbitrary'),
        cost_estimate=cost(4 * tokens * m * n, 4 * tokens * n + 8 * m * n + 4 * tokens * m),
        name='norm_partial',
    )((first * (tiles // 2)).astype(jnp.int32).reshape(1), dyg, dyu, wg, wu)
    return out


def lane_fold(v):
    parts = [v[:, k:k + 128] for k in range(0, v.shape[1], 128)]
    while len(parts) > 1:
        parts = [p + q for p, q in zip(parts[::2], parts[1::2])] + parts[len(parts) & ~1:]
    return parts[0]


def direction(g, r_ref, rows, c_ref):
    r = r_ref[rows, :]
    r = jnp.concatenate([r] * (g.shape[1] // 128), axis=1)
    return g * lax.rsqrt(r * c_ref[...])


def square_kernel(row_total, sizes, hyper_ref, g0, g1, g2, all_ref, r_ref,
                  c0, c1, c2, w0, w1, w2, n0, n1, n2, ratio_ref, part_ref, acc_ref):
    step = pl.program_id(0)
    beta_two = hyper_ref[0]
    grads, c_new = (g0, g1, g2), (n0, n1, n2)
    starts = [0, sizes[0], sizes[0] + sizes[1]]

    @pl.when(step == 0)
    def _():
        off = 0
        for c_old, new, total in zip((c0, c1, c2), c_new, row_total):
            size = c_old.shape[1]
            new[...] = beta_two * c_old[...] + (1.0 - beta_two) * (all_ref[:, off:off + size] / total)
            off += size
        for k in range(3):
            mean = jnp.sum(all_ref[:, off + 128 * k:off + 128 * k + 128], axis=1, keepdims=True) / row_total[k]
            for i in range(starts[k], starts[k] + sizes[k], 128):
                ratio_ref[i:i + 128, :] = jnp.broadcast_to(r_ref[:, i:i + 128] / mean, (128, 128)).T
        acc_ref[...] = jnp.zeros_like(acc_ref)

    for k in range(3):
        tile = grads[k].shape[0]

        @pl.loop(0, tile // 8, unroll=4)
        def _(i):
            g = grads[k][pl.ds(pl.multiple_of(i * 8, 8), 8), :]
            rows = pl.ds(pl.multiple_of(starts[k] + step * tile + i * 8, 8), 8)
            u = direction(g, ratio_ref, rows, c_new[k])
            acc_ref[k] += lane_fold(u * u)

    @pl.when(step == pl.num_programs(0) - 1)
    def _():
        part_ref[...] = jnp.zeros_like(part_ref)
        for k in range(3):
            part_ref[k:k + 1, :] = jnp.sum(acc_ref[k], axis=0, keepdims=True)
        for k, w in enumerate((w0, w1, w2)):
            part_ref[3 + k:4 + k, :] = jnp.sum(lane_fold(w[...]), axis=0, keepdims=True)


def square_sums(hyper_params, grads, all_sums, r_new, c_old, w_sq, row_total):
    steps = 8
    whole = lambda v: pl.BlockSpec(v.shape, lambda i: (0, 0))
    in_specs = (
        [pl.BlockSpec(memory_space=pltpu.SMEM)]
        + [pl.BlockSpec((g.shape[0] // steps, g.shape[1]), lambda i: (i, 0)) for g in grads]
        + [whole(v) for v in (all_sums, r_new, *c_old, *w_sq)]
    )
    out_shape = [jax.ShapeDtypeStruct(c.shape, F32) for c in c_old] + [
        jax.ShapeDtypeStruct((r_new.shape[1], 128), F32),
        jax.ShapeDtypeStruct((8, 128), F32),
    ]
    size = sum(g.size for g in grads)
    out = pl.pallas_call(
        functools.partial(square_kernel, row_total, [g.shape[0] for g in grads]),
        grid=(steps,),
        in_specs=in_specs,
        out_specs=[whole(v) for v in out_shape],
        out_shape=out_shape,
        scratch_shapes=[pltpu.VMEM((3, 8, 128), F32)],
        compiler_params=params('arbitrary'),
        cost_estimate=cost(1000 * size, 4 * size),
        name='square_sums',
    )(hyper_params, *grads, all_sums, r_new, *c_old, *w_sq)
    return out[:3], out[3], out[4]


def act_kernel(pieces, total, row_ref, hyper_ref, dya_ref, *refs):
    piece_refs, refs = refs[:pieces], refs[pieces:]
    wa_ref, wb_ref, refs = refs[0], refs[1], refs[2:]
    weights, grads, c_new, (ratio_ref, sum_ref) = refs[:3], refs[3:6], refs[6:9], refs[9:11]
    out_ref, new, (acc_ref, scale_ref, dyb_ref, sems) = refs[11], refs[12:15], refs[15:]
    step = pl.program_id(0)
    slot = lax.rem(step, 2)

    def fetch(i):
        source = lax.bitwise_xor(i, row_ref[0])
        for k, piece in enumerate(piece_refs):
            @pl.when(source == k)
            def _():
                pltpu.make_async_copy(piece, dyb_ref.at[lax.rem(i, 2)], sems.at[lax.rem(i, 2)]).start()

    @pl.when(step == 0)
    def _():
        fetch(step)
        mean = jnp.sum(sum_ref[...], axis=1, keepdims=True) / total
        for k in range(3):
            rms_u, rms_w = jnp.sqrt(mean[k:k + 1]), jnp.sqrt(mean[3 + k:4 + k])
            scale = hyper_ref[1] * jnp.maximum(EPS_TWO, rms_w) / jnp.maximum(1.0, rms_u / hyper_ref[2])
            scale_ref[k] = jnp.broadcast_to(scale, (8, 128))

    @pl.when(step + 1 < pl.num_programs(0))
    def _():
        fetch(step + 1)

    @pl.when(step >= 0)
    def _():
        acc_ref[...] = lax.dot_general(dya_ref[...], wa_ref[...], NT, preferred_element_type=F32)

    pltpu.make_async_copy(piece_refs[0], dyb_ref.at[slot], sems.at[slot]).wait()

    @pl.when(step < pl.num_programs(0))
    def _():
        other = lax.dot_general(dyb_ref[slot], wb_ref[...], NT, preferred_element_type=F32)
        out_ref[...] = (acc_ref[...] + other).astype(BF16)

    start = 0
    for k in range(3):
        tile, n = weights[k].shape

        @pl.loop(0, tile // 8, unroll=4)
        def _(i):
            slab = pl.ds(pl.multiple_of(i * 8, 8), 8)
            rows = pl.ds(pl.multiple_of(start + step * tile + i * 8, 8), 8)
            u = direction(grads[k][slab, :], ratio_ref, rows, c_new[k])
            scale = jnp.concatenate([scale_ref[k]] * (n // 128), axis=1)
            new[k][slab, :] = weights[k][slab, :] - scale * u

        start += tile * pl.num_programs(0)


def act_and_update(hyper_params, row, dya, pieces, wa, wb, weights, grads, c_new, ratio, sums, total):
    tile = pieces[0].shape[0]
    tokens, n = dya.shape
    steps = tokens // tile
    m = wa.shape[0]
    fixed = lambda v: pl.BlockSpec(v.shape, lambda i: (0, 0), pipeline_mode=pl.Buffered(1))
    rows = lambda v: pl.BlockSpec((v.shape[0] // steps, v.shape[1]), lambda i: (i, 0))
    size = sum(w.size for w in weights)
    out = pl.pallas_call(
        functools.partial(act_kernel, len(pieces), total),
        grid=(steps,),
        in_specs=[pl.BlockSpec(memory_space=pltpu.SMEM)] * 2
        + [rows(dya)]
        + [pl.BlockSpec(memory_space=pl.ANY)] * len(pieces)
        + [fixed(wa), fixed(wb)]
        + [rows(v) for v in (*weights, *grads)]
        + [fixed(v) for v in (*c_new, ratio, sums)],
        out_specs=[pl.BlockSpec((tile, m), lambda i: (i, 0))] + [rows(w) for w in weights],
        out_shape=[jax.ShapeDtypeStruct((tokens, m), BF16)] + [jax.ShapeDtypeStruct(w.shape, F32) for w in weights],
        scratch_shapes=[
            pltpu.VMEM((tile, m), F32),
            pltpu.VMEM((3, 8, 128), F32),
            pltpu.VMEM((2, tile, n), BF16),
            pltpu.SemaphoreType.DMA((2,)),
        ],
        compiler_params=params('arbitrary'),
        cost_estimate=cost(4 * tokens * m * n, 4 * tokens * n + 4 * m * n + 2 * tokens * m + 12 * size),
        name='act_and_update',
    )(row.astype(jnp.int32).reshape(1), hyper_params, dya, *pieces, wa, wb, *weights, *grads, *c_new, ratio, sums)
    return out[0], out[1:]


def swap_col(v):
    return lax.ppermute(v, 'col', [(0, 1), (1, 0)])


def swap_row(v, row_size, mask):
    return lax.ppermute(v, 'row', [(i, i ^ mask) for i in range(row_size)])


def sum_row(v, row_size):
    step = row_size // 2
    while step:
        v = v + swap_row(v, row_size, step)
        step //= 2
    return v


def solution(mesh):
    row_size = mesh.shape['row']
    col_size = mesh.shape['col']
    weight_spec = P('row', 'col')
    act_spec = P(None, 'row')
    grad_spec = P(None, 'col')
    in_specs = (weight_spec,) * 3 + (act_spec, act_spec) + (grad_spec,) * 3 + (P('row'), P('col')) * 3 + (P(),)
    out_specs = (weight_spec,) * 3 + (P('row'), P('col')) * 3 + (act_spec, act_spec)

    def body(w_gate, w_up, w_down, x_norm, x_act, dy_gate, dy_up, dy_down, r_gate, c_gate, r_up, c_up, r_down, c_down, hyper_params):
        row = lax.axis_index('row')
        col = lax.axis_index('col')
        tokens = x_norm.shape[0]
        half = tokens // col_size
        beta_two = hyper_params[0]

        share = tokens // row_size
        piece = lax.dynamic_slice_in_dim(dy_down, row * share, share, axis=0)
        pieces = {0: swap_col(piece)}
        b_down, w_sq_down = cast_weight(w_down)
        o_down = swap_col(b_down)
        (g_gate, row_gate, col_gate), (g_up, row_up, col_up) = weight_grads(x_norm, [dy_gate, dy_up], 512)
        for mask in range(2, row_size, 2):
            pieces[mask] = swap_row(pieces[0], row_size, mask)
        part = (half // 8, half // 2 - half // 8, half - half // 2)
        sent_a, sent_b, sent_c, own_ab, own_c, w_sq_gate, w_sq_up = norm_partial(
            1 - col, dy_gate, dy_up, w_gate, w_up, (*part, half // 2, half // 2))
        got_a = swap_col(sent_a)
        ((g_down, row_down, col_down),) = weight_grads(x_act, [dy_down], 512)
        row_all = jnp.concatenate([row_gate, row_up, row_down], axis=1)
        row_peer = swap_col(row_all)
        got_b = swap_col(sent_b)
        for mask in range(0, row_size, 2):
            pieces[mask + 1] = swap_row(pieces[mask], row_size, 1)

        sizes = [r_gate.shape[0], r_up.shape[0], r_down.shape[0]]
        bounds = [0, sizes[0], sizes[0] + sizes[1], sum(sizes)]
        row_total = [v * row_size for v in sizes]
        col_total = [v.shape[0] * col_size for v in (c_gate, c_up, c_down)]
        index = lax.broadcasted_iota(jnp.int32, row_all.shape, 1)
        length = jnp.where(index < bounds[1], col_total[0], jnp.where(index < bounds[2], col_total[1], col_total[2]))
        r_old = jnp.concatenate([r_gate, r_up, r_down])[None]
        r_new = beta_two * r_old + (1.0 - beta_two) * ((row_all + row_peer) / length.astype(F32))
        r_part = [lane_fold(r_new[:, bounds[k]:bounds[k + 1]]) for k in range(3)]
        all_sums = sum_row(jnp.concatenate([col_gate, col_up, col_down, *r_part], axis=1), row_size)
        grads = [g_gate, g_up, g_down]
        c_new, ratio, sums = square_sums(
            hyper_params, grads, all_sums, r_new, [c_gate[None], c_up[None], c_down[None]],
            [w_sq_gate, w_sq_up, w_sq_down], row_total)
        sums = sum_row(sums, row_size)
        sums_peer = swap_col(sums)
        got_c = swap_col(sent_c)
        dx_act, new = act_and_update(
            hyper_params, row, dy_down, [pieces[k] for k in range(row_size)], b_down, o_down,
            [w_gate, w_up, w_down], grads, c_new, ratio, sums + sums_peer, float(row_total[0] * col_total[0]))
        r_new = [r_new[0, bounds[k]:bounds[k + 1]] for k in range(3)]
        c_new = [c[0] for c in c_new]

        mine_ab = (own_ab + jnp.concatenate([got_a, got_b])).astype(BF16)
        theirs_ab = swap_col(mine_ab)
        mine_c = (own_c + got_c).astype(BF16)
        theirs_c = swap_col(mine_c)
        dx_norm = jnp.where(
            col == 0,
            jnp.concatenate([mine_ab, mine_c, theirs_ab, theirs_ab]),
            jnp.concatenate([theirs_ab, theirs_ab, mine_ab, mine_c]),
        )
        dx_norm = lax.dynamic_update_slice_in_dim(dx_norm, theirs_c, (1 - col) * half + half // 2, axis=0)
        return (*new, r_new[0], c_new[0], r_new[1], c_new[1], r_new[2], c_new[2], dx_norm, dx_act)

    return jax.shard_map(body, mesh=mesh, in_specs=in_specs, out_specs=out_specs, check_vma=False)
```

```python
import functools

import jax
import jax.numpy as jnp
from jax import lax
from jax.experimental import pallas as pl
from jax.experimental.pallas import tpu as pltpu
from jax.sharding import PartitionSpec as P


EPS_ONE = 1e-30
EPS_TWO = 1e-3
F32 = jnp.float32
BF16 = jnp.bfloat16
VMEM_LIMIT = 60 * 1024 * 1024
NT = (((1,), (1,)), ((), ()))


def params(*semantics):
    return pltpu.CompilerParams(dimension_semantics=semantics, vmem_limit_bytes=VMEM_LIMIT)


def cost(flops, nbytes):
    return pl.CostEstimate(flops=int(flops), bytes_accessed=int(nbytes), transcendentals=0)


def fold_squares(v):
    return jnp.sum((v * v).reshape(v.shape[0] // 8, 8, v.shape[1]), axis=0)


def cast_kernel(w_ref, b_ref, s_ref):
    w = w_ref[...]
    b_ref[...] = w.astype(BF16)

    @pl.when(pl.program_id(0) == 0)
    def _():
        s_ref[...] = jnp.zeros_like(s_ref)

    s_ref[...] += fold_squares(w)


def cast_weight(w):
    rows, cols = w.shape
    tile = 256
    return pl.pallas_call(
        cast_kernel,
        grid=(rows // tile,),
        in_specs=[pl.BlockSpec((tile, cols), lambda i: (i, 0))],
        out_specs=[pl.BlockSpec((tile, cols), lambda i: (i, 0)), pl.BlockSpec((8, cols), lambda i: (0, 0))],
        out_shape=[jax.ShapeDtypeStruct((rows, cols), BF16), jax.ShapeDtypeStruct((8, cols), F32)],
        compiler_params=params('arbitrary'),
        cost_estimate=cost(w.size * 1000, w.size * 6),
        name='cast_weight',
    )(w)


def grad_block(xt_ref, dy_ref, g_ref, row_ref, col_ref):
    g = jnp.dot(xt_ref[...], dy_ref[...], preferred_element_type=F32)
    g_ref[...] = g
    q = g * g + EPS_ONE
    col_ref[...] = jnp.sum(q, axis=0, keepdims=True)
    part = q[:, :128]
    for k in range(1, q.shape[1] // 128):
        part += q[:, k * 128:(k + 1) * 128]
    row_ref[...] += part


def grad_kernel(count, steps, x_ref, *refs):
    dy, out, xt_ref, part_ref = refs[:count], refs[count:-2], refs[-2], refs[-1]
    step = pl.program_id(0)

    @pl.when(step == 0)
    def _():
        xt_ref[...] = x_ref[...].T

    for k in range(count):
        @pl.when(step == k * steps)
        def _():
            part_ref[...] = jnp.zeros_like(part_ref)

        @pl.when((step >= k * steps) & (step < (k + 1) * steps))
        def _():
            grad_block(xt_ref, dy[k], out[3 * k], part_ref, out[3 * k + 2])

        @pl.when(step == (k + 1) * steps - 1)
        def _():
            out[3 * k + 1][...] = jnp.sum(part_ref[...].T, axis=0, keepdims=True)


def weight_grads(x, dys, tile):
    tokens, m = x.shape
    n = dys[0].shape[1]
    steps = n // tile
    count = len(dys)

    def block(k):
        return lambda j: (0, jnp.clip(j - k * steps, 0, steps - 1))

    out_specs, out_shape = [], []
    for k in range(count):
        out_specs += [
            pl.BlockSpec((m, tile), block(k)),
            pl.BlockSpec((1, m), lambda j: (0, 0)),
            pl.BlockSpec((1, tile), block(k)),
        ]
        out_shape += [
            jax.ShapeDtypeStruct((m, n), F32),
            jax.ShapeDtypeStruct((1, m), F32),
            jax.ShapeDtypeStruct((1, n), F32),
        ]
    out = pl.pallas_call(
        functools.partial(grad_kernel, count, steps),
        grid=(steps * count,),
        in_specs=[pl.BlockSpec((tokens, m), lambda j: (0, 0), pipeline_mode=pl.Buffered(1))]
        + [pl.BlockSpec((tokens, tile), block(k)) for k in range(count)],
        out_specs=out_specs,
        out_shape=out_shape,
        scratch_shapes=[pltpu.VMEM((m, tokens), BF16), pltpu.VMEM((m, 128), F32)],
        compiler_params=params('arbitrary'),
        cost_estimate=cost(2 * count * tokens * m * n, count * (2 * tokens * (m + n) + 4 * m * n)),
        name='weight_grads',
    )(x, *dys)
    return [tuple(out[3 * k:3 * k + 3]) for k in range(count)]


def norm_kernel(chunk, start_ref, dyg_ref, dyu_ref, wg_ref, wu_ref, *refs):
    out, squares, (acc_ref, wb_ref, stage_ref, sems) = refs[:-6], refs[-6:-4], refs[-4:]
    step = pl.program_id(0)
    weights = (wg_ref, wu_ref)
    chunks = wg_ref.shape[1] // chunk
    slots = stage_ref.shape[0]
    tile = dyg_ref.shape[0]

    def fetch(matrix, c):
        slot = lax.rem(matrix * chunks + c, slots)
        cols = pl.ds(pl.multiple_of(c * chunk, chunk), chunk)
        return pltpu.make_async_copy(weights[matrix].at[:, cols], stage_ref.at[slot], sems.at[slot])

    @pl.when(step == 0)
    def _():
        for c in range(slots):
            fetch(0, c).start()
        acc_ref[...] = jnp.zeros_like(acc_ref)
        for k, dy_ref in enumerate((dyg_ref, dyu_ref)):
            squares[k][...] = jnp.zeros_like(squares[k])

            @pl.loop(0, chunks)
            def _(c):
                fetch(k, c).wait()
                slot = lax.rem(k * chunks + c, slots)
                cols = pl.ds(pl.multiple_of(c * chunk, chunk), chunk)
                w = stage_ref[slot]
                wb_ref[k, :, cols] = w.astype(BF16)
                squares[k][...] += fold_squares(w)

                @pl.when(c + slots < chunks)
                def _():
                    fetch(k, c + slots).start()

                if k == 0:
                    @pl.when(c + slots >= chunks)
                    def _():
                        fetch(1, c + slots - chunks).start()

                acc_ref[...] += lax.dot_general(dy_ref[:, cols], wb_ref[k, :, cols], NT, preferred_element_type=F32)

    @pl.when(step > 0)
    def _():
        acc_ref[...] = lax.dot_general(dyg_ref[...], wb_ref[0], NT, preferred_element_type=F32) + lax.dot_general(
            dyu_ref[...], wb_ref[1], NT, preferred_element_type=F32)

    at = 0
    for ref in out:
        for lo in range(at - at % tile, at + ref.shape[0], tile):
            first, last = max(lo, at), min(lo + tile, at + ref.shape[0])

            @pl.when(step == lo // tile)
            def _():
                ref[first - at:last - at, :] = acc_ref[first - lo:last - lo, :]

        at += ref.shape[0]


def norm_partial(first, dyg, dyu, wg, wu, counts):
    tile, chunk, slots = 512, 1024, 3
    tokens, n = dyg.shape
    m = wg.shape[0]
    tiles = tokens // tile
    dy_spec = pl.BlockSpec((tile, n), lambda i, start: (lax.rem(i + start[0], tiles), 0))
    any_spec = pl.BlockSpec(memory_space=pl.ANY)

    out = pl.pallas_call(
        functools.partial(norm_kernel, chunk),
        grid_spec=pltpu.PrefetchScalarGridSpec(
            num_scalar_prefetch=1,
            grid=(tiles,),
            in_specs=[dy_spec, dy_spec, any_spec, any_spec],
            out_specs=[pl.BlockSpec((c, m), lambda i, start: (0, 0)) for c in counts]
            + [pl.BlockSpec((8, chunk), lambda i, start: (0, 0))] * 2,
            scratch_shapes=[
                pltpu.VMEM((tile, m), F32),
                pltpu.VMEM((2, m, n), BF16),
                pltpu.VMEM((slots, m, chunk), F32),
                pltpu.SemaphoreType.DMA((slots,)),
            ],
        ),
        out_shape=[jax.ShapeDtypeStruct((c, m), F32) for c in counts] + [jax.ShapeDtypeStruct((8, chunk), F32)] * 2,
        compiler_params=params('arbitrary'),
        cost_estimate=cost(4 * tokens * m * n, 4 * tokens * n + 8 * m * n + 4 * tokens * m),
        name='norm_partial',
    )((first * (tiles // 2)).astype(jnp.int32).reshape(1), dyg, dyu, wg, wu)
    return out


def lane_fold(v):
    parts = [v[:, k:k + 128] for k in range(0, v.shape[1], 128)]
    while len(parts) > 1:
        parts = [p + q for p, q in zip(parts[::2], parts[1::2])] + parts[len(parts) & ~1:]
    return parts[0]


def direction(g, r_ref, rows, c_ref):
    r = r_ref[rows, :]
    r = jnp.concatenate([r] * (g.shape[1] // 128), axis=1)
    return g * lax.rsqrt(r * c_ref[...])


def square_kernel(row_total, sizes, hyper_ref, g0, g1, g2, all_ref, r_ref,
                  c0, c1, c2, w0, w1, w2, n0, n1, n2, ratio_ref, part_ref, acc_ref):
    step = pl.program_id(0)
    beta_two = hyper_ref[0]
    grads, c_new = (g0, g1, g2), (n0, n1, n2)
    starts = [0, sizes[0], sizes[0] + sizes[1]]

    @pl.when(step == 0)
    def _():
        off = 0
        for c_old, new, total in zip((c0, c1, c2), c_new, row_total):
            size = c_old.shape[1]
            new[...] = beta_two * c_old[...] + (1.0 - beta_two) * (all_ref[:, off:off + size] / total)
            off += size
        for k in range(3):
            mean = jnp.sum(all_ref[:, off + 128 * k:off + 128 * k + 128], axis=1, keepdims=True) / row_total[k]
            for i in range(starts[k], starts[k] + sizes[k], 128):
                ratio_ref[i:i + 128, :] = jnp.broadcast_to(r_ref[:, i:i + 128] / mean, (128, 128)).T
        acc_ref[...] = jnp.zeros_like(acc_ref)

    for k in range(3):
        tile = grads[k].shape[0]

        @pl.loop(0, tile // 8, unroll=4)
        def _(i):
            g = grads[k][pl.ds(pl.multiple_of(i * 8, 8), 8), :]
            rows = pl.ds(pl.multiple_of(starts[k] + step * tile + i * 8, 8), 8)
            u = direction(g, ratio_ref, rows, c_new[k])
            acc_ref[k] += lane_fold(u * u)

    @pl.when(step == pl.num_programs(0) - 1)
    def _():
        part_ref[...] = jnp.zeros_like(part_ref)
        for k in range(3):
            part_ref[k:k + 1, :] = jnp.sum(acc_ref[k], axis=0, keepdims=True)
        for k, w in enumerate((w0, w1, w2)):
            part_ref[3 + k:4 + k, :] = jnp.sum(lane_fold(w[...]), axis=0, keepdims=True)


def square_sums(hyper_params, grads, all_sums, r_new, c_old, w_sq, row_total):
    steps = 4
    whole = lambda v: pl.BlockSpec(v.shape, lambda i: (0, 0))
    in_specs = (
        [pl.BlockSpec(memory_space=pltpu.SMEM)]
        + [pl.BlockSpec((g.shape[0] // steps, g.shape[1]), lambda i: (i, 0)) for g in grads]
        + [whole(v) for v in (all_sums, r_new, *c_old, *w_sq)]
    )
    out_shape = [jax.ShapeDtypeStruct(c.shape, F32) for c in c_old] + [
        jax.ShapeDtypeStruct((r_new.shape[1], 128), F32),
        jax.ShapeDtypeStruct((8, 128), F32),
    ]
    size = sum(g.size for g in grads)
    out = pl.pallas_call(
        functools.partial(square_kernel, row_total, [g.shape[0] for g in grads]),
        grid=(steps,),
        in_specs=in_specs,
        out_specs=[whole(v) for v in out_shape],
        out_shape=out_shape,
        scratch_shapes=[pltpu.VMEM((3, 8, 128), F32)],
        compiler_params=params('arbitrary'),
        cost_estimate=cost(1000 * size, 4 * size),
        name='square_sums',
    )(hyper_params, *grads, all_sums, r_new, *c_old, *w_sq)
    return out[:3], out[3], out[4]


def act_kernel(pieces, total, row_ref, hyper_ref, dya_ref, *refs):
    piece_refs, refs = refs[:pieces], refs[pieces:]
    wa_ref, wb_hbm, refs = refs[0], refs[1], refs[2:]
    weights, grads, c_new, (ratio_ref, sum_ref) = refs[:3], refs[3:6], refs[6:9], refs[9:11]
    out_ref, new, (acc_ref, scale_ref, dyb_ref, wb_ref, sems, w_sem) = refs[11], refs[12:15], refs[15:]
    step = pl.program_id(0)
    slot = lax.rem(step, 2)

    def fetch(i):
        source = lax.bitwise_xor(i, row_ref[0])
        for k, piece in enumerate(piece_refs):
            @pl.when(source == k)
            def _():
                pltpu.make_async_copy(piece, dyb_ref.at[lax.rem(i, 2)], sems.at[lax.rem(i, 2)]).start()

    w_copy = pltpu.make_async_copy(wb_hbm, wb_ref, w_sem)

    @pl.when(step == 0)
    def _():
        fetch(step)
        w_copy.start()
        mean = jnp.sum(sum_ref[...], axis=1, keepdims=True) / total
        for k in range(3):
            rms_u, rms_w = jnp.sqrt(mean[k:k + 1]), jnp.sqrt(mean[3 + k:4 + k])
            scale = hyper_ref[1] * jnp.maximum(EPS_TWO, rms_w) / jnp.maximum(1.0, rms_u / hyper_ref[2])
            scale_ref[k] = jnp.broadcast_to(scale, (8, 128))

    @pl.when(step + 1 < pl.num_programs(0))
    def _():
        fetch(step + 1)

    @pl.when(step >= 0)
    def _():
        acc_ref[...] = lax.dot_general(dya_ref[...], wa_ref[...], NT, preferred_element_type=F32)

    pltpu.make_async_copy(piece_refs[0], dyb_ref.at[slot], sems.at[slot]).wait()

    @pl.when(step == 0)
    def _():
        w_copy.wait()

    @pl.when(step < pl.num_programs(0))
    def _():
        other = lax.dot_general(dyb_ref[slot], wb_ref[...], NT, preferred_element_type=F32)
        out_ref[...] = (acc_ref[...] + other).astype(BF16)

    start = 0
    for k in range(3):
        tile, n = weights[k].shape

        @pl.loop(0, tile // 8, unroll=4)
        def _(i):
            slab = pl.ds(pl.multiple_of(i * 8, 8), 8)
            rows = pl.ds(pl.multiple_of(start + step * tile + i * 8, 8), 8)
            u = direction(grads[k][slab, :], ratio_ref, rows, c_new[k])
            scale = jnp.concatenate([scale_ref[k]] * (n // 128), axis=1)
            new[k][slab, :] = weights[k][slab, :] - scale * u

        start += tile * pl.num_programs(0)


def act_and_update(hyper_params, row, dya, pieces, wa, wb, weights, grads, c_new, ratio, sums, total):
    tile = pieces[0].shape[0]
    tokens, n = dya.shape
    steps = tokens // tile
    m = wa.shape[0]
    fixed = lambda v: pl.BlockSpec(v.shape, lambda i: (0, 0), pipeline_mode=pl.Buffered(1))
    rows = lambda v: pl.BlockSpec((v.shape[0] // steps, v.shape[1]), lambda i: (i, 0))
    size = sum(w.size for w in weights)
    out = pl.pallas_call(
        functools.partial(act_kernel, len(pieces), total),
        grid=(steps,),
        in_specs=[pl.BlockSpec(memory_space=pltpu.SMEM)] * 2
        + [rows(dya)]
        + [pl.BlockSpec(memory_space=pl.ANY)] * len(pieces)
        + [fixed(wa), pl.BlockSpec(memory_space=pl.ANY)]
        + [rows(v) for v in (*weights, *grads)]
        + [fixed(v) for v in (*c_new, ratio, sums)],
        out_specs=[pl.BlockSpec((tile, m), lambda i: (i, 0))] + [rows(w) for w in weights],
        out_shape=[jax.ShapeDtypeStruct((tokens, m), BF16)] + [jax.ShapeDtypeStruct(w.shape, F32) for w in weights],
        scratch_shapes=[
            pltpu.VMEM((tile, m), F32),
            pltpu.VMEM((3, 8, 128), F32),
            pltpu.VMEM((2, tile, n), BF16),
            pltpu.VMEM((m, n), BF16),
            pltpu.SemaphoreType.DMA((2,)),
            pltpu.SemaphoreType.DMA,
        ],
        compiler_params=params('arbitrary'),
        cost_estimate=cost(4 * tokens * m * n, 4 * tokens * n + 4 * m * n + 2 * tokens * m + 12 * size),
        name='act_and_update',
    )(row.astype(jnp.int32).reshape(1), hyper_params, dya, *pieces, wa, wb, *weights, *grads, *c_new, ratio, sums)
    return out[0], out[1:]


def swap_col(v):
    return lax.ppermute(v, 'col', [(0, 1), (1, 0)])


def swap_row(v, row_size, mask):
    return lax.ppermute(v, 'row', [(i, i ^ mask) for i in range(row_size)])


def sum_row(v, row_size):
    x, y, far = (swap_row(v, row_size, mask) for mask in (2, 4, 6))
    v = (v + x) + (y + far)
    return v + swap_row(v, row_size, 1)


def solution(mesh):
    row_size = mesh.shape['row']
    col_size = mesh.shape['col']
    weight_spec = P('row', 'col')
    act_spec = P(None, 'row')
    grad_spec = P(None, 'col')
    in_specs = (weight_spec,) * 3 + (act_spec, act_spec) + (grad_spec,) * 3 + (P('row'), P('col')) * 3 + (P(),)
    out_specs = (weight_spec,) * 3 + (P('row'), P('col')) * 3 + (act_spec, act_spec)

    def body(w_gate, w_up, w_down, x_norm, x_act, dy_gate, dy_up, dy_down, r_gate, c_gate, r_up, c_up, r_down, c_down, hyper_params):
        row = lax.axis_index('row')
        col = lax.axis_index('col')
        tokens = x_norm.shape[0]
        half = tokens // col_size
        beta_two = hyper_params[0]

        share = tokens // row_size
        piece = lax.dynamic_slice_in_dim(dy_down, row * share, share, axis=0)
        pieces = {0: swap_col(piece)}
        b_down, w_sq_down = cast_weight(w_down)
        o_down = swap_col(b_down)
        (g_gate, row_gate, col_gate), (g_up, row_up, col_up) = weight_grads(x_norm, [dy_gate, dy_up], 512)
        for mask in range(2, row_size, 2):
            pieces[mask] = swap_row(pieces[0], row_size, mask)
        ahead = 1120
        part = (256, ahead - 256, half - ahead)
        sent_a, sent_b, sent_c, own_ab, own_c, w_sq_gate, w_sq_up = norm_partial(
            1 - col, dy_gate, dy_up, w_gate, w_up, (*part, ahead, half - ahead))
        got_a = swap_col(sent_a)
        ((g_down, row_down, col_down),) = weight_grads(x_act, [dy_down], 512)
        row_all = jnp.concatenate([row_gate, row_up, row_down], axis=1)
        row_peer = swap_col(row_all)
        got_b = swap_col(sent_b)
        for mask in range(0, row_size, 2):
            pieces[mask + 1] = swap_row(pieces[mask], row_size, 1)

        sizes = [r_gate.shape[0], r_up.shape[0], r_down.shape[0]]
        bounds = [0, sizes[0], sizes[0] + sizes[1], sum(sizes)]
        row_total = [v * row_size for v in sizes]
        col_total = [v.shape[0] * col_size for v in (c_gate, c_up, c_down)]
        index = lax.broadcasted_iota(jnp.int32, row_all.shape, 1)
        length = jnp.where(index < bounds[1], col_total[0], jnp.where(index < bounds[2], col_total[1], col_total[2]))
        r_old = jnp.concatenate([r_gate, r_up, r_down])[None]
        r_new = beta_two * r_old + (1.0 - beta_two) * ((row_all + row_peer) / length.astype(F32))
        r_part = [lane_fold(r_new[:, bounds[k]:bounds[k + 1]]) for k in range(3)]
        all_sums = sum_row(jnp.concatenate([col_gate, col_up, col_down, *r_part], axis=1), row_size)
        grads = [g_gate, g_up, g_down]
        c_new, ratio, sums = square_sums(
            hyper_params, grads, all_sums, r_new, [c_gate[None], c_up[None], c_down[None]],
            [w_sq_gate, w_sq_up, w_sq_down], row_total)
        sums = sum_row(sums, row_size)
        sums_peer = swap_col(sums)
        got_c = swap_col(sent_c)
        dx_act, new = act_and_update(
            hyper_params, row, dy_down, [pieces[k] for k in range(row_size)], b_down, o_down,
            [w_gate, w_up, w_down], grads, c_new, ratio, sums + sums_peer, float(row_total[0] * col_total[0]))
        r_new = [r_new[0, bounds[k]:bounds[k + 1]] for k in range(3)]
        c_new = [c[0] for c in c_new]

        mine_ab = (own_ab + jnp.concatenate([got_a, got_b])).astype(BF16)
        theirs_ab = swap_col(mine_ab)
        mine_c = (own_c + got_c).astype(BF16)
        theirs_c = swap_col(mine_c)
        dx_norm = jnp.where(
            col == 0,
            jnp.concatenate([mine_ab, mine_c, theirs_ab, mine_c]),
            jnp.concatenate([theirs_ab, mine_c, mine_ab, mine_c]),
        )
        dx_norm = lax.dynamic_update_slice_in_dim(dx_norm, theirs_c, (1 - col) * half + ahead, axis=0)
        return (*new, r_new[0], c_new[0], r_new[1], c_new[1], r_new[2], c_new[2], dx_norm, dx_act)

    return jax.shard_map(body, mesh=mesh, in_specs=in_specs, out_specs=out_specs, check_vma=False)
```

```python
import functools

import jax
import jax.numpy as jnp
from jax import lax
from jax.experimental import pallas as pl
from jax.experimental.pallas import tpu as pltpu
from jax.sharding import PartitionSpec as P


EPS_ONE = 1e-30
EPS_TWO = 1e-3
F32 = jnp.float32
BF16 = jnp.bfloat16
VMEM_LIMIT = 60 * 1024 * 1024
NT = (((1,), (1,)), ((), ()))


def params(*semantics):
    return pltpu.CompilerParams(dimension_semantics=semantics, vmem_limit_bytes=VMEM_LIMIT)


def cost(flops, nbytes):
    return pl.CostEstimate(flops=int(flops), bytes_accessed=int(nbytes), transcendentals=0)


def fold_squares(v):
    return jnp.sum((v * v).reshape(v.shape[0] // 8, 8, v.shape[1]), axis=0)


def cast_kernel(w_ref, b_ref, s_ref):
    w = w_ref[...]
    b_ref[...] = w.astype(BF16)

    @pl.when(pl.program_id(0) == 0)
    def _():
        s_ref[...] = jnp.zeros_like(s_ref)

    s_ref[...] += fold_squares(w)


def cast_weight(w):
    rows, cols = w.shape
    tile = 256
    return pl.pallas_call(
        cast_kernel,
        grid=(rows // tile,),
        in_specs=[pl.BlockSpec((tile, cols), lambda i: (i, 0))],
        out_specs=[pl.BlockSpec((tile, cols), lambda i: (i, 0)), pl.BlockSpec((8, cols), lambda i: (0, 0))],
        out_shape=[jax.ShapeDtypeStruct((rows, cols), BF16), jax.ShapeDtypeStruct((8, cols), F32)],
        compiler_params=params('arbitrary'),
        cost_estimate=cost(w.size * 1000, w.size * 6),
        name='cast_weight',
    )(w)


def grad_block(xt_ref, dy_ref, g_ref, row_ref, col_ref):
    g = jnp.dot(xt_ref[...], dy_ref[...], preferred_element_type=F32)
    g_ref[...] = g
    q = g * g + EPS_ONE
    col_ref[...] = jnp.sum(q, axis=0, keepdims=True)
    part = q[:, :128]
    for k in range(1, q.shape[1] // 128):
        part += q[:, k * 128:(k + 1) * 128]
    row_ref[...] += part


def grad_kernel(count, steps, x_ref, *refs):
    dy, grads, (row_ref, col_ref, xt_ref, part_ref) = refs[:count], refs[count:-4], refs[-4:]
    step = pl.program_id(0)

    @pl.when(step == 0)
    def _():
        xt_ref[...] = x_ref[...].T

    for k in range(count):
        @pl.when(step == k * steps)
        def _():
            part_ref[...] = jnp.zeros_like(part_ref)

        @pl.when((step >= k * steps) & (step < (k + 1) * steps))
        def _():
            grad_block(xt_ref, dy[k], grads[k], part_ref, col_ref)

        @pl.when(step == (k + 1) * steps - 1)
        def _():
            row_ref[...] = jnp.sum(part_ref[...].T, axis=0, keepdims=True)


def weight_grads(x, dys, tile):
    tokens, m = x.shape
    n = dys[0].shape[1]
    steps = n // tile
    count = len(dys)

    def block(k):
        return lambda j: (0, jnp.clip(j - k * steps, 0, steps - 1))

    out_specs = [pl.BlockSpec((m, tile), block(k)) for k in range(count)] + [
        pl.BlockSpec((1, m), lambda j: (0, j // steps)),
        pl.BlockSpec((1, tile), lambda j: (0, j)),
    ]
    out_shape = [jax.ShapeDtypeStruct((m, n), F32)] * count + [
        jax.ShapeDtypeStruct((1, m * count), F32),
        jax.ShapeDtypeStruct((1, n * count), F32),
    ]
    return pl.pallas_call(
        functools.partial(grad_kernel, count, steps),
        grid=(steps * count,),
        in_specs=[pl.BlockSpec((tokens, m), lambda j: (0, 0), pipeline_mode=pl.Buffered(1))]
        + [pl.BlockSpec((tokens, tile), block(k)) for k in range(count)],
        out_specs=out_specs,
        out_shape=out_shape,
        scratch_shapes=[pltpu.VMEM((m, tokens), BF16), pltpu.VMEM((m, 128), F32)],
        compiler_params=params('arbitrary'),
        cost_estimate=cost(2 * count * tokens * m * n, count * (2 * tokens * (m + n) + 4 * m * n)),
        name='weight_grads',
    )(x, *dys)


def norm_kernel(chunk, start_ref, dyg_ref, dyu_ref, wg_ref, wu_ref, *refs):
    out, squares, (acc_ref, wb_ref, stage_ref, sems) = refs[:-6], refs[-6:-4], refs[-4:]
    step = pl.program_id(0)
    weights = (wg_ref, wu_ref)
    chunks = wg_ref.shape[1] // chunk
    slots = stage_ref.shape[0]
    tile = dyg_ref.shape[0]

    def fetch(matrix, c):
        slot = lax.rem(matrix * chunks + c, slots)
        cols = pl.ds(pl.multiple_of(c * chunk, chunk), chunk)
        return pltpu.make_async_copy(weights[matrix].at[:, cols], stage_ref.at[slot], sems.at[slot])

    @pl.when(step == 0)
    def _():
        for c in range(slots):
            fetch(0, c).start()
        acc_ref[...] = jnp.zeros_like(acc_ref)
        for k, dy_ref in enumerate((dyg_ref, dyu_ref)):
            squares[k][...] = jnp.zeros_like(squares[k])

            @pl.loop(0, chunks)
            def _(c):
                fetch(k, c).wait()
                slot = lax.rem(k * chunks + c, slots)
                cols = pl.ds(pl.multiple_of(c * chunk, chunk), chunk)
                w = stage_ref[slot]
                wb_ref[k, :, cols] = w.astype(BF16)
                squares[k][...] += fold_squares(w)

                @pl.when(c + slots < chunks)
                def _():
                    fetch(k, c + slots).start()

                if k == 0:
                    @pl.when(c + slots >= chunks)
                    def _():
                        fetch(1, c + slots - chunks).start()

                acc_ref[...] += lax.dot_general(dy_ref[:, cols], wb_ref[k, :, cols], NT, preferred_element_type=F32)

    @pl.when(step > 0)
    def _():
        acc_ref[...] = lax.dot_general(dyg_ref[...], wb_ref[0], NT, preferred_element_type=F32) + lax.dot_general(
            dyu_ref[...], wb_ref[1], NT, preferred_element_type=F32)

    at = 0
    for ref in out:
        for lo in range(at - at % tile, at + ref.shape[0], tile):
            first, last = max(lo, at), min(lo + tile, at + ref.shape[0])

            @pl.when(step == lo // tile)
            def _():
                ref[first - at:last - at, :] = acc_ref[first - lo:last - lo, :]

        at += ref.shape[0]


def norm_partial(first, dyg, dyu, wg, wu, counts):
    tile, chunk, slots = 512, 1024, 3
    tokens, n = dyg.shape
    m = wg.shape[0]
    tiles = tokens // tile
    dy_spec = pl.BlockSpec((tile, n), lambda i, start: (lax.rem(i + start[0], tiles), 0))
    any_spec = pl.BlockSpec(memory_space=pl.ANY)

    out = pl.pallas_call(
        functools.partial(norm_kernel, chunk),
        grid_spec=pltpu.PrefetchScalarGridSpec(
            num_scalar_prefetch=1,
            grid=(tiles,),
            in_specs=[dy_spec, dy_spec, any_spec, any_spec],
            out_specs=[pl.BlockSpec((c, m), lambda i, start: (0, 0)) for c in counts]
            + [pl.BlockSpec((8, chunk), lambda i, start: (0, 0))] * 2,
            scratch_shapes=[
                pltpu.VMEM((tile, m), F32),
                pltpu.VMEM((2, m, n), BF16),
                pltpu.VMEM((slots, m, chunk), F32),
                pltpu.SemaphoreType.DMA((slots,)),
            ],
        ),
        out_shape=[jax.ShapeDtypeStruct((c, m), F32) for c in counts] + [jax.ShapeDtypeStruct((8, chunk), F32)] * 2,
        compiler_params=params('arbitrary'),
        cost_estimate=cost(4 * tokens * m * n, 4 * tokens * n + 8 * m * n + 4 * tokens * m),
        name='norm_partial',
    )((first * (tiles // 2)).astype(jnp.int32).reshape(1), dyg, dyu, wg, wu)
    return out


def lane_fold(v):
    parts = [v[:, k:k + 128] for k in range(0, v.shape[1], 128)]
    while len(parts) > 1:
        parts = [p + q for p, q in zip(parts[::2], parts[1::2])] + parts[len(parts) & ~1:]
    return parts[0]


def direction(g, r_ref, rows, c_ref):
    r = r_ref[rows, :]
    r = jnp.concatenate([r] * (g.shape[1] // 128), axis=1)
    return g * lax.rsqrt(r * c_ref[...])


def square_kernel(row_total, sizes, hyper_ref, g0, g1, g2, all_ref, r_ref,
                  c0, c1, c2, w0, w1, w2, n0, n1, n2, ratio_ref, part_ref, acc_ref):
    step = pl.program_id(0)
    beta_two = hyper_ref[0]
    grads, c_new = (g0, g1, g2), (n0, n1, n2)
    starts = [0, sizes[0], sizes[0] + sizes[1]]

    @pl.when(step == 0)
    def _():
        off = 0
        for c_old, new, total in zip((c0, c1, c2), c_new, row_total):
            size = c_old.shape[1]
            new[...] = beta_two * c_old[...] + (1.0 - beta_two) * (all_ref[:, off:off + size] / total)
            off += size
        for k in range(3):
            mean = jnp.sum(all_ref[:, off + 128 * k:off + 128 * k + 128], axis=1, keepdims=True) / row_total[k]
            for i in range(starts[k], starts[k] + sizes[k], 128):
                ratio_ref[i:i + 128, :] = jnp.broadcast_to(r_ref[:, i:i + 128] / mean, (128, 128)).T
        acc_ref[...] = jnp.zeros_like(acc_ref)

    for k in range(3):
        tile = grads[k].shape[0]

        @pl.loop(0, tile // 8, unroll=4)
        def _(i):
            g = grads[k][pl.ds(pl.multiple_of(i * 8, 8), 8), :]
            rows = pl.ds(pl.multiple_of(starts[k] + step * tile + i * 8, 8), 8)
            u = direction(g, ratio_ref, rows, c_new[k])
            acc_ref[k] += lane_fold(u * u)

    @pl.when(step == pl.num_programs(0) - 1)
    def _():
        part_ref[...] = jnp.zeros_like(part_ref)
        for k in range(3):
            part_ref[k:k + 1, :] = jnp.sum(acc_ref[k], axis=0, keepdims=True)
        for k, w in enumerate((w0, w1, w2)):
            part_ref[3 + k:4 + k, :] = jnp.sum(lane_fold(w[...]), axis=0, keepdims=True)


def square_sums(hyper_params, grads, all_sums, r_new, c_old, w_sq, row_total):
    steps = 4
    whole = lambda v: pl.BlockSpec(v.shape, lambda i: (0, 0))
    in_specs = (
        [pl.BlockSpec(memory_space=pltpu.SMEM)]
        + [pl.BlockSpec((g.shape[0] // steps, g.shape[1]), lambda i: (i, 0)) for g in grads]
        + [whole(v) for v in (all_sums, r_new, *c_old, *w_sq)]
    )
    out_shape = [jax.ShapeDtypeStruct(c.shape, F32) for c in c_old] + [
        jax.ShapeDtypeStruct((r_new.shape[1], 128), F32),
        jax.ShapeDtypeStruct((8, 128), F32),
    ]
    size = sum(g.size for g in grads)
    out = pl.pallas_call(
        functools.partial(square_kernel, row_total, [g.shape[0] for g in grads]),
        grid=(steps,),
        in_specs=in_specs,
        out_specs=[whole(v) for v in out_shape],
        out_shape=out_shape,
        scratch_shapes=[pltpu.VMEM((3, 8, 128), F32)],
        compiler_params=params('arbitrary'),
        cost_estimate=cost(1000 * size, 4 * size),
        name='square_sums',
    )(hyper_params, *grads, all_sums, r_new, *c_old, *w_sq)
    return out[:3], out[3], out[4]


def act_kernel(pieces, total, row_ref, hyper_ref, dya_ref, *refs):
    piece_refs, refs = refs[:pieces], refs[pieces:]
    wa_ref, wb_hbm, refs = refs[0], refs[1], refs[2:]
    weights, grads, c_new, (ratio_ref, sum_ref) = refs[:3], refs[3:6], refs[6:9], refs[9:11]
    out_ref, new, (acc_ref, scale_ref, dyb_ref, wb_ref, sems, w_sem) = refs[11], refs[12:15], refs[15:]
    step = pl.program_id(0)
    slot = lax.rem(step, 2)

    def fetch(i):
        source = lax.bitwise_xor(i, row_ref[0])
        for k, piece in enumerate(piece_refs):
            @pl.when(source == k)
            def _():
                pltpu.make_async_copy(piece, dyb_ref.at[lax.rem(i, 2)], sems.at[lax.rem(i, 2)]).start()

    w_copy = pltpu.make_async_copy(wb_hbm, wb_ref, w_sem)

    @pl.when(step == 0)
    def _():
        fetch(step)
        w_copy.start()
        mean = jnp.sum(sum_ref[...], axis=1, keepdims=True) / total
        for k in range(3):
            rms_u, rms_w = jnp.sqrt(mean[k:k + 1]), jnp.sqrt(mean[3 + k:4 + k])
            scale = hyper_ref[1] * jnp.maximum(EPS_TWO, rms_w) / jnp.maximum(1.0, rms_u / hyper_ref[2])
            scale_ref[k] = jnp.broadcast_to(scale, (8, 128))

    @pl.when(step + 1 < pl.num_programs(0))
    def _():
        fetch(step + 1)

    @pl.when(step >= 0)
    def _():
        acc_ref[...] = lax.dot_general(dya_ref[...], wa_ref[...], NT, preferred_element_type=F32)

    pltpu.make_async_copy(piece_refs[0], dyb_ref.at[slot], sems.at[slot]).wait()

    @pl.when(step == 0)
    def _():
        w_copy.wait()

    @pl.when(step < pl.num_programs(0))
    def _():
        other = lax.dot_general(dyb_ref[slot], wb_ref[...], NT, preferred_element_type=F32)
        out_ref[...] = (acc_ref[...] + other).astype(BF16)

    start = 0
    for k in range(3):
        tile, n = weights[k].shape

        @pl.loop(0, tile // 8, unroll=4)
        def _(i):
            slab = pl.ds(pl.multiple_of(i * 8, 8), 8)
            rows = pl.ds(pl.multiple_of(start + step * tile + i * 8, 8), 8)
            u = direction(grads[k][slab, :], ratio_ref, rows, c_new[k])
            scale = jnp.concatenate([scale_ref[k]] * (n // 128), axis=1)
            new[k][slab, :] = weights[k][slab, :] - scale * u

        start += tile * pl.num_programs(0)


def act_and_update(hyper_params, row, dya, pieces, wa, wb, weights, grads, c_new, ratio, sums, total):
    tile = pieces[0].shape[0]
    tokens, n = dya.shape
    steps = tokens // tile
    m = wa.shape[0]
    fixed = lambda v: pl.BlockSpec(v.shape, lambda i: (0, 0), pipeline_mode=pl.Buffered(1))
    rows = lambda v: pl.BlockSpec((v.shape[0] // steps, v.shape[1]), lambda i: (i, 0))
    size = sum(w.size for w in weights)
    out = pl.pallas_call(
        functools.partial(act_kernel, len(pieces), total),
        grid=(steps,),
        in_specs=[pl.BlockSpec(memory_space=pltpu.SMEM)] * 2
        + [rows(dya)]
        + [pl.BlockSpec(memory_space=pl.ANY)] * len(pieces)
        + [fixed(wa), pl.BlockSpec(memory_space=pl.ANY)]
        + [rows(v) for v in (*weights, *grads)]
        + [fixed(v) for v in (*c_new, ratio, sums)],
        out_specs=[pl.BlockSpec((tile, m), lambda i: (i, 0))] + [rows(w) for w in weights],
        out_shape=[jax.ShapeDtypeStruct((tokens, m), BF16)] + [jax.ShapeDtypeStruct(w.shape, F32) for w in weights],
        scratch_shapes=[
            pltpu.VMEM((tile, m), F32),
            pltpu.VMEM((3, 8, 128), F32),
            pltpu.VMEM((2, tile, n), BF16),
            pltpu.VMEM((m, n), BF16),
            pltpu.SemaphoreType.DMA((2,)),
            pltpu.SemaphoreType.DMA,
        ],
        compiler_params=params('arbitrary'),
        cost_estimate=cost(4 * tokens * m * n, 4 * tokens * n + 4 * m * n + 2 * tokens * m + 12 * size),
        name='act_and_update',
    )(row.astype(jnp.int32).reshape(1), hyper_params, dya, *pieces, wa, wb, *weights, *grads, *c_new, ratio, sums)
    return out[0], out[1:]


def swap_col(v):
    return lax.ppermute(v, 'col', [(0, 1), (1, 0)])


def swap_row(v, row_size, mask):
    return lax.ppermute(v, 'row', [(i, i ^ mask) for i in range(row_size)])


def sum_row(v, row_size):
    x, y, far = (swap_row(v, row_size, mask) for mask in (2, 4, 6))
    v = (v + x) + (y + far)
    return v + swap_row(v, row_size, 1)


def solution(mesh):
    row_size = mesh.shape['row']
    col_size = mesh.shape['col']
    weight_spec = P('row', 'col')
    act_spec = P(None, 'row')
    grad_spec = P(None, 'col')
    in_specs = (weight_spec,) * 3 + (act_spec, act_spec) + (grad_spec,) * 3 + (P('row'), P('col')) * 3 + (P(),)
    out_specs = (weight_spec,) * 3 + (P('row'), P('col')) * 3 + (act_spec, act_spec)

    def body(w_gate, w_up, w_down, x_norm, x_act, dy_gate, dy_up, dy_down, r_gate, c_gate, r_up, c_up, r_down, c_down, hyper_params):
        row = lax.axis_index('row')
        col = lax.axis_index('col')
        tokens = x_norm.shape[0]
        half = tokens // col_size
        beta_two = hyper_params[0]

        share = tokens // row_size
        piece = lax.dynamic_slice_in_dim(dy_down, row * share, share, axis=0)
        pieces = {0: swap_col(piece)}
        b_down, w_sq_down = cast_weight(w_down)
        o_down = swap_col(b_down)
        g_gate, g_up, row_in, col_in = weight_grads(x_norm, [dy_gate, dy_up], 512)
        for mask in range(2, row_size, 2):
            pieces[mask] = swap_row(pieces[0], row_size, mask)
        ahead = 992
        part = (224, ahead - 224, half - ahead)
        sent_a, sent_b, sent_c, own_ab, own_c, w_sq_gate, w_sq_up = norm_partial(
            1 - col, dy_gate, dy_up, w_gate, w_up, (*part, ahead, half - ahead))
        got_a = swap_col(sent_a)
        g_down, row_down, col_down = weight_grads(x_act, [dy_down], 512)
        row_all = jnp.concatenate([row_in, row_down], axis=1)
        row_peer = swap_col(row_all)
        got_b = swap_col(sent_b)
        for mask in range(0, row_size, 2):
            pieces[mask + 1] = swap_row(pieces[mask], row_size, 1)

        sizes = [r_gate.shape[0], r_up.shape[0], r_down.shape[0]]
        bounds = [0, sizes[0], sizes[0] + sizes[1], sum(sizes)]
        row_total = [v * row_size for v in sizes]
        col_total = [v.shape[0] * col_size for v in (c_gate, c_up, c_down)]
        index = lax.broadcasted_iota(jnp.int32, row_all.shape, 1)
        length = jnp.where(index < bounds[1], col_total[0], jnp.where(index < bounds[2], col_total[1], col_total[2]))
        r_old = jnp.concatenate([r_gate, r_up, r_down])[None]
        r_new = beta_two * r_old + (1.0 - beta_two) * ((row_all + row_peer) / length.astype(F32))
        r_part = [lane_fold(r_new[:, bounds[k]:bounds[k + 1]]) for k in range(3)]
        all_sums = sum_row(jnp.concatenate([col_in, col_down, *r_part], axis=1), row_size)
        grads = [g_gate, g_up, g_down]
        c_new, ratio, sums = square_sums(
            hyper_params, grads, all_sums, r_new, [c_gate[None], c_up[None], c_down[None]],
            [w_sq_gate, w_sq_up, w_sq_down], row_total)
        sums = sum_row(sums, row_size)
        sums_peer = swap_col(sums)
        got_c = swap_col(sent_c)
        dx_act, new = act_and_update(
            hyper_params, row, dy_down, [pieces[k] for k in range(row_size)], b_down, o_down,
            [w_gate, w_up, w_down], grads, c_new, ratio, sums + sums_peer, float(row_total[0] * col_total[0]))
        r_new = [r_new[0, bounds[k]:bounds[k + 1]] for k in range(3)]
        c_new = [c[0] for c in c_new]

        mine_ab = (own_ab + jnp.concatenate([got_a, got_b])).astype(BF16)
        theirs_ab = swap_col(mine_ab)
        mine_c = (own_c + got_c).astype(BF16)
        theirs_c = swap_col(mine_c)
        dx_norm = jnp.where(
            col == 0,
            jnp.concatenate([mine_ab, mine_c, theirs_ab, mine_c]),
            jnp.concatenate([theirs_ab, mine_c, mine_ab, mine_c]),
        )
        dx_norm = lax.dynamic_update_slice_in_dim(dx_norm, theirs_c, (1 - col) * half + ahead, axis=0)
        return (*new, r_new[0], c_new[0], r_new[1], c_new[1], r_new[2], c_new[2], dx_norm, dx_act)

    return jax.shard_map(body, mesh=mesh, in_specs=in_specs, out_specs=out_specs, check_vma=False)
```
